128 devices in a mesh: section: 4 (over z), dp: 32 (over y, x, core).
Axes of the slice: x: 4, y: 4, z: 4, core: 2. Of those that a mesh axis runs over, the one named last changes fastest.
Arguments:
- images: bfloat16 [2, 6304, 1024], P(None, 'dp'), may hold values from -44 to 44
- cotangent: bfloat16 [2, 6304, 1024], P(None, 'dp'), may hold values from -0.75 to 0.75
- w_in: bfloat16 [4, 1024, 2048], P('section'), may hold values from -0.1875 to 0.1875
- w_out: bfloat16 [4, 2048, 1024], P('section'), may hold values from -0.125 to 0.125
- gain: float32 [4, 1024], P('section'), may hold values from 0.5 to 1.5
- shift: float32 [4, 1024], P('section'), may hold values from -3 to 3
Outputs:
- section_outputs: bfloat16 [4, 2, 6304, 1024], P('section', None, 'dp')
- input_grads: bfloat16 [4, 2, 6304, 1024], P('section', None, 'dp')
- grad_w_in: float32 [4, 1024, 2048], P('section', 'dp')
- grad_w_out: float32 [4, 2048, 1024], P('section', 'dp')
- grad_gain: float32 [4, 1024], P('section')
- grad_shift: float32 [4, 1024], P('section')
The draws below stay inside these ranges and needn't reach their ends.
All inputs are finite; a program needn't handle non-finite values.
Results may differ from the reference program's by a relative error of at most 0.0095.
Values may be sent and summed in bfloat16 or wider, within the bound.
No kernel may reach another device: no remote copies, remote signals or barrier semaphores. Data moves between devices by JAX's collectives and lax.ppermute only.
A program may use at most 192 MiB of HBM per device.

```python
import jax
import jax.numpy as jnp
from jax import lax

D = 1024
FF = 2048
PATCHES = 197
IMG = 1
MICRO = 2
TOKENS = 6304
SECTIONS = 4
N_DP = 32


def draw_images(key, part):
    keys = jax.random.split(jax.random.fold_in(key, 11), 2)
    positions = jnp.arange(TOKENS)
    block = (positions // (IMG * PATCHES)).astype(jnp.float32)
    spread = max(N_DP - 1, 1)
    centre = jnp.clip(0.5 * jax.random.normal(keys[1], (D,), jnp.float32), -2.0, 2.0)
    noise = jnp.clip(jax.random.normal(keys[0], (MICRO, TOKENS, D), jnp.float32), -4.0, 4.0)
    level = 1.0 + 2.0 * block / spread
    column = jnp.ones((D,), jnp.float32)
    values = centre + level[None, :, None] * column * noise
    return values.astype(jnp.bfloat16)


def raised(entries, key, source, target, blocks, factor):
    owner, partner = [(jnp.arange(entries.shape[position]) // (entries.shape[position] // blocks)).reshape([-1 if axis == position else 1 for axis in range(entries.ndim)]) for position in (source, target)]
    chosen = jax.random.permutation(key, blocks)[partner]
    strong = (owner == chosen) | (owner == (partner + blocks // 2) % blocks)
    return jnp.where(strong, factor * entries, entries)


def block_levels(stream_key, extent, cuts, low, high):
    level, own = 1.0, jax.random.fold_in(stream_key, 6)
    for dim, shards_of in cuts:
        heights = jnp.exp(jax.random.uniform(jax.random.fold_in(own, dim), (shards_of,), jnp.float32, low / len(cuts), high / len(cuts)))
        level = level * jnp.repeat(heights, extent[dim] // shards_of).reshape([-1 if axis == dim else 1 for axis in range(len(extent))])
    return level


def bell_draw(stream_key, shape, scale, most, shards=(), dtype=jnp.bfloat16):
    drawn = jax.random.normal(stream_key, shape, jnp.float32) * scale
    if len(shards) > 0:
        drawn = block_levels(stream_key, shape, shards, -0.22, 0.18) * drawn
    return jnp.clip(drawn, min=-most, max=most).astype(dtype)


def bell_draw_with(key, shape, scale, most, pieces, heavy, held_as=jnp.bfloat16):
    result = scale * jax.random.normal(key, shape, jnp.float32)
    if pieces:
        result = result * block_levels(key, shape, pieces, -0.22, 0.18)
    return jnp.clip(raised(result, jax.random.fold_in(key, 3), *heavy), -most, most).astype(held_as)


def setup_inputs(seed: int = 0) -> dict:
    key_of = jax.random.split(jax.random.key(seed), 7)
    images = draw_images(jax.random.fold_in(key_of[6], 71), 0)
    cotangent = bell_draw_with(key_of[1], (MICRO, TOKENS, D), 0.125, 0.75, ((1, 32),), (1, 2, 32, 2.75))
    w_in = bell_draw(key_of[2], (SECTIONS, D, FF), D ** -0.5, 0.1875, ((0, 4),))
    w_out = bell_draw(key_of[3], (SECTIONS, FF, D), FF ** -0.5, 0.125, ((0, 4),))
    gain = jnp.clip(1.0 + 0.1 * jax.random.normal(key_of[4], (SECTIONS, D), jnp.float32), 0.5, 1.5)
    shift = bell_draw(key_of[5], (SECTIONS, D), 0.5, 3.0, ((0, 4),), jnp.float32)
    return dict(images=images, cotangent=cotangent, w_in=w_in, w_out=w_out, gain=gain, shift=shift)


epsilon = 1e-05
gelu_scale = 0.7978845608028654
cubic_term = 0.044715

def gelu_parts(before):
    inner = gelu_scale * (before + cubic_term * before * before * before)
    bend = jnp.tanh(inner)
    value = 0.5 * before * (1.0 + bend)
    slope = 0.5 * (1.0 + bend) + 0.5 * before * (1.0 - bend * bend) * gelu_scale * (1.0 + 3.0 * cubic_term * before * before)
    return (value, slope)

def reference(images, cotangent, w_in, w_out, gain, shift):
    sections = w_in.shape[0]
    micro = images.shape[0]
    rows = images.shape[1]
    outputs = [[None] * micro for layer in range(sections)]
    in_grads = [[None] * micro for layer in range(sections)]
    stored = {}
    for batch in range(micro):
        inputs = images[batch]
        for layer in range(sections):
            inputs_f = inputs.astype(jnp.float32)
            mean = lax.optimization_barrier(jnp.sum(inputs_f, axis=0)) / rows
            centered = inputs_f - mean
            spread = lax.optimization_barrier(jnp.sum(centered * centered, axis=0)) / rows
            inverse = lax.rsqrt(spread + epsilon)
            normed = centered * inverse
            affine = (normed * gain[layer] + shift[layer]).astype(jnp.bfloat16)
            before = jnp.dot(affine, w_in[layer], preferred_element_type=jnp.float32)
            value, slope = gelu_parts(before)
            active = value.astype(jnp.bfloat16)
            output = (inputs_f + jnp.dot(active, w_out[layer], preferred_element_type=jnp.float32)).astype(jnp.bfloat16)
            stored[layer, batch] = (normed, inverse, affine, slope, active)
            outputs[layer][batch] = output
            inputs = output
    grad_in = [jnp.zeros(w_in.shape[1:], jnp.float32) for layer in range(sections)]
    grad_out = [jnp.zeros(w_out.shape[1:], jnp.float32) for layer in range(sections)]
    grad_gain = [jnp.zeros(gain.shape[1:], jnp.float32) for layer in range(sections)]
    grad_shift = [jnp.zeros(gain.shape[1:], jnp.float32) for layer in range(sections)]
    for batch in range(micro):
        upstream = cotangent[batch]
        for layer in reversed(range(sections)):
            normed, inverse, affine, slope, active = stored[layer, batch]
            grad_out[layer] = grad_out[layer] + jnp.dot(active.T, upstream, preferred_element_type=jnp.float32)
            grad_active = jnp.dot(upstream, w_out[layer].T, preferred_element_type=jnp.float32)
            grad_before = (grad_active * slope).astype(jnp.bfloat16)
            grad_in[layer] = grad_in[layer] + jnp.dot(affine.T, grad_before, preferred_element_type=jnp.float32)
            grad_affine = jnp.dot(grad_before, w_in[layer].T, preferred_element_type=jnp.float32)
            sum_grad = lax.optimization_barrier(jnp.sum(grad_affine, axis=0))
            sum_cross = lax.optimization_barrier(jnp.sum(grad_affine * normed, axis=0))
            grad_gain[layer] = grad_gain[layer] + sum_cross
            grad_shift[layer] = grad_shift[layer] + sum_grad
            grad_norm = inverse * gain[layer] * (grad_affine - sum_grad / rows - normed * sum_cross / rows)
            upstream = (upstream.astype(jnp.float32) + grad_norm).astype(jnp.bfloat16)
            in_grads[layer][batch] = upstream
    section_outputs = jnp.stack([jnp.stack(column) for column in outputs])
    input_grads = jnp.stack([jnp.stack(column) for column in in_grads])
    return (section_outputs, input_grads, jnp.stack(grad_in), jnp.stack(grad_out), jnp.stack(grad_gain), jnp.stack(grad_shift))
```

```python
import jax
import jax.numpy as jnp
from jax import lax
from jax.experimental import pallas as pl
from jax.experimental.pallas import tpu as pltpu
from jax.sharding import PartitionSpec as P

epsilon = 1e-05
gelu_scale = 0.7978845608028654
cubic_term = 0.044715
f32 = jnp.float32
bf16 = jnp.bfloat16


def gelu_parts(before):
    square = before * before
    inner = gelu_scale * (before + cubic_term * square * before)
    bend = jnp.tanh(inner)
    half = 0.5 * (1.0 + bend)
    value = before * half
    slope = half + 0.5 * before * (1.0 - bend * bend) * gelu_scale * (1.0 + 3.0 * cubic_term * square)
    return (value, slope)


def params(mib=59):
    return pltpu.CompilerParams(dimension_semantics=("arbitrary",), vmem_limit_bytes=mib * 1024 * 1024)


def row_mask(padded, rows):
    return lax.broadcasted_iota(jnp.int32, (padded, 1), 0) < rows


def moments(x, rows):
    total = jnp.sum(x, axis=0, keepdims=True)
    off = x - total / rows
    return total, jnp.sum(off * off, axis=0, keepdims=True)


def keep_padded(ref, x):
    rows = x.shape[0]
    whole = rows - rows % 8
    ref[whole:, :] = jnp.zeros((ref.shape[0] - whole, ref.shape[1]), ref.dtype)
    ref[:rows, :] = x


def fill_copies(ref, rows_of):
    for i, row in enumerate(rows_of):
        ref[:, i : i + 1, :] = jnp.broadcast_to(row[None], (ref.shape[0], 1, row.shape[1]))


def image_stats(images, copies):
    micro, rows, width = images.shape

    def kernel(x_ref, out_ref):
        parts = []
        for m in range(micro):
            parts += list(moments(x_ref[m].astype(f32), rows))
        fill_copies(out_ref, parts)

    return pl.pallas_call(
        kernel,
        grid=(1,),
        in_specs=[pl.BlockSpec((micro, rows, width), lambda i: (0, 0, 0))],
        out_specs=pl.BlockSpec((copies, 2 * micro, width), lambda i: (0, 0, 0)),
        out_shape=jax.ShapeDtypeStruct((copies, 2 * micro, width), f32),
        compiler_params=params(8),
        name="image_stats",
    )(images)


def combine_stats(arrived, rows, rows_local):
    copies, twice, width = arrived.shape

    def kernel(a_ref, out_ref):
        for m in range(twice // 2):
            sums = a_ref[:, 2 * m, :]
            mean = jnp.sum(sums, axis=0, keepdims=True) / rows
            off = sums / rows_local - mean
            squares = jnp.sum(a_ref[:, 2 * m + 1, :], axis=0, keepdims=True)
            squares = squares + rows_local * jnp.sum(off * off, axis=0, keepdims=True)
            out_ref[m, 0:1, :] = mean
            out_ref[m, 1:2, :] = lax.rsqrt(squares / rows + epsilon)

    return pl.pallas_call(
        kernel,
        grid=(1,),
        in_specs=[pl.BlockSpec(arrived.shape, lambda i: (0, 0, 0))],
        out_specs=pl.BlockSpec((twice // 2, 2, width), lambda i: (0, 0, 0)),
        out_shape=jax.ShapeDtypeStruct((twice // 2, 2, width), f32),
        compiler_params=params(8),
        name="combine_stats",
    )(arrived)


def forward(where, images, arrived, stats_img, stats_arr, gain, shift, w_in, w_out, bufs, copies, padded):
    _, rows, width = images.shape
    hidden = w_in.shape[2]
    block = 512
    steps = hidden // block

    def kernel(at, img, arr, simg, sarr, g, sh, win, wout, *rest):
        rest = rest[len(bufs) :]
        xb, stb, affb, actb, slb, outb, send, part, x_s, aff_s, acc = rest
        j = pl.program_id(0)
        mask = row_mask(padded, rows)

        @pl.when(j == 0)
        def _():
            first = at[1] == 1
            x = jnp.where(first, img[0].astype(f32), arr[...].astype(f32))
            keep_padded(x_s, x)
            xb[0] = x.astype(bf16)
            x = x_s[...]
            st = jnp.where(first, simg[0], sarr[0])
            affine = (x - st[0:1]) * st[1:2] * g[...] + sh[...]
            affine = jnp.where(mask, affine, 0.0).astype(bf16)
            aff_s[...] = affine
            affb[0] = affine
            stb[0] = st

        before = jnp.dot(aff_s[...], win[0], preferred_element_type=f32)
        value, slope = gelu_parts(before)
        active = value.astype(bf16)
        actb[0] = active
        slb[0] = slope
        grown = jnp.dot(active, wout[0], preferred_element_type=f32)

        @pl.when(j == 0)
        def _():
            acc[...] = x_s[...] + grown

        @pl.when((j > 0) & (j < steps - 1))
        def _():
            acc[...] += grown

        @pl.when(j == steps - 1)
        def _():
            output = (acc[...] + grown)[:rows].astype(bf16)
            outb[0] = output
            send[...] = output
            fill_copies(part, moments(output.astype(f32), rows))

    fixed = lambda shape: pl.BlockSpec(shape, lambda j, at: tuple(0 for _ in shape))
    slot = lambda shape: pl.BlockSpec(shape, lambda j, at: (at[0], 0, 0))
    out_shape = [
        jax.ShapeDtypeStruct((3, rows, width), bf16),
        jax.ShapeDtypeStruct((3, 2, width), f32),
        jax.ShapeDtypeStruct((3, padded, width), bf16),
        jax.ShapeDtypeStruct((3, padded, hidden), bf16),
        jax.ShapeDtypeStruct((3, padded, hidden), f32),
        jax.ShapeDtypeStruct((3, rows, width), bf16),
        jax.ShapeDtypeStruct((rows, width), bf16),
        jax.ShapeDtypeStruct((copies, 2, width), f32),
    ]
    in_specs = [
        pl.BlockSpec((1, rows, width), lambda j, at: (at[2], 0, 0)),
        fixed((rows, width)),
        pl.BlockSpec((1, 2, width), lambda j, at: (at[2], 0, 0)),
        fixed((1, 2, width)),
        fixed((1, width)),
        fixed((1, width)),
        pl.BlockSpec((1, width, block), lambda j, at: (0, 0, j)),
        pl.BlockSpec((1, block, width), lambda j, at: (0, j, 0)),
    ]
    out = pl.pallas_call(
        kernel,
        out_shape=out_shape,
        grid_spec=pltpu.PrefetchScalarGridSpec(
            num_scalar_prefetch=1,
            grid=(steps,),
            in_specs=in_specs + [pl.BlockSpec(memory_space=pl.ANY)] * len(bufs),
            out_specs=[
                slot((1, rows, width)),
                slot((1, 2, width)),
                slot((1, padded, width)),
                pl.BlockSpec((1, padded, block), lambda j, at: (at[0], 0, j)),
                pl.BlockSpec((1, padded, block), lambda j, at: (at[0], 0, j)),
                slot((1, rows, width)),
                fixed((rows, width)),
                fixed((copies, 2, width)),
            ],
            scratch_shapes=[
                pltpu.VMEM((padded, width), f32),
                pltpu.VMEM((padded, width), bf16),
                pltpu.VMEM((padded, width), f32),
            ],
        ),
        input_output_aliases={9 + i: i for i in range(len(bufs))},
        compiler_params=params(),
        name="section_forward",
    )(where, images, arrived, stats_img, stats_arr, gain, shift, w_in, w_out, *bufs)
    return list(out[:6]), out[6], out[7]


def backward(where, cotangent, arrived, fix, gain, w_in, w_out, kept, bufs, copies, padded):
    _, rows, width = cotangent.shape
    hidden = w_in.shape[2]
    block = 512
    steps = hidden // block
    xb, stb, slb, outb = kept

    def kernel(at, cot, arr, fx, g, win, wout, x_ref, st, slope, own, *rest):
        rest = rest[len(bufs) :]
        upb, gbb, ub, send, part, up_s, sum_s, acc = rest
        j = pl.program_id(0)

        @pl.when(j == 0)
        def _():
            last = at[1] == 1
            high = jnp.where(last, cot[0].astype(f32), arr[...].astype(f32))
            low = -fx[0:1] - fx[1:2] * (own[0].astype(f32) - fx[2:3])
            low = jnp.where(last, 0.0, low)
            keep_padded(acc, high)
            up_s[:, :width] = acc[...].astype(bf16)
            keep_padded(acc, low)
            up_s[:, width:] = acc[...].astype(bf16)
            upb[0] = up_s[...]
            sum_s[...] = high + low

        contract = (((1,), (1,)), ((), ()))
        grad_active = lax.dot_general(up_s[:, :width], wout[0], contract, preferred_element_type=f32)
        grad_active += lax.dot_general(up_s[:, width:], wout[0], contract, preferred_element_type=f32)
        grad_before = (grad_active * slope[0]).astype(bf16)
        gbb[0] = grad_before
        grown = lax.dot_general(grad_before, win[0], contract, preferred_element_type=f32)

        @pl.when(j == 0)
        def _():
            acc[...] = grown

        @pl.when((j > 0) & (j < steps - 1))
        def _():
            acc[...] += grown

        @pl.when(j == steps - 1)
        def _():
            grad_affine = (acc[...] + grown)[:rows]
            inverse = st[0, 1:2, :]
            normed = (x_ref[0].astype(f32) - st[0, 0:1, :]) * inverse
            sum_grad = jnp.sum(grad_affine, axis=0, keepdims=True)
            sum_cross = jnp.sum(grad_affine * normed, axis=0, keepdims=True)
            u = sum_s[...] + inverse * g[...] * grad_affine
            ub[0] = u
            send[...] = u.astype(bf16)
            fill_copies(part, (sum_grad, sum_cross))

    fixed = lambda shape: pl.BlockSpec(shape, lambda j, at: tuple(0 for _ in shape))
    slot = lambda shape: pl.BlockSpec(shape, lambda j, at: (at[0], 0, 0))
    in_specs = [
        pl.BlockSpec((1, rows, width), lambda j, at: (at[2], 0, 0)),
        fixed((rows, width)),
        fixed((3, width)),
        fixed((1, width)),
        pl.BlockSpec((1, width, block), lambda j, at: (0, 0, j)),
        pl.BlockSpec((1, block, width), lambda j, at: (0, j, 0)),
        slot((1, rows, width)),
        slot((1, 2, width)),
        pl.BlockSpec((1, padded, block), lambda j, at: (at[0], 0, j)),
        slot((1, rows, width)),
    ]
    out = pl.pallas_call(
        kernel,
        out_shape=[
            jax.ShapeDtypeStruct((3, padded, 2 * width), bf16),
            jax.ShapeDtypeStruct((3, padded, hidden), bf16),
            jax.ShapeDtypeStruct((3, rows, width), f32),
            jax.ShapeDtypeStruct((rows, width), bf16),
            jax.ShapeDtypeStruct((copies, 2, width), f32),
        ],
        grid_spec=pltpu.PrefetchScalarGridSpec(
            num_scalar_prefetch=1,
            grid=(steps,),
            in_specs=in_specs + [pl.BlockSpec(memory_space=pl.ANY)] * len(bufs),
            out_specs=[
                slot((1, padded, 2 * width)),
                pl.BlockSpec((1, padded, block), lambda j, at: (at[0], 0, j)),
                slot((1, rows, width)),
                fixed((rows, width)),
                fixed((copies, 2, width)),
            ],
            scratch_shapes=[
                pltpu.VMEM((padded, 2 * width), bf16),
                pltpu.VMEM((rows, width), f32),
                pltpu.VMEM((padded, width), f32),
            ],
        ),
        input_output_aliases={11 + i: i for i in range(len(bufs))},
        compiler_params=params(),
        name="section_backward",
    )(where, cotangent, arrived, fix, gain, w_in, w_out, xb, stb, slb, outb, *bufs)
    return list(out[:3]), out[3], out[4]


def combine_grads(where, arrived, stb, gain, rows):
    copies, _, width = arrived.shape

    def kernel(at, a_ref, st, g, fix, sums):
        sum_grad = jnp.sum(a_ref[:, 0, :], axis=0, keepdims=True)
        sum_cross = jnp.sum(a_ref[:, 1, :], axis=0, keepdims=True)
        inverse = st[0, 1:2, :]
        scale = inverse * g[...]
        fix[0:1, :] = scale * (sum_grad / rows)
        fix[1:2, :] = scale * inverse * (sum_cross / rows)
        fix[2:3, :] = st[0, 0:1, :]
        sums[0:1, :] = sum_cross
        sums[1:2, :] = sum_grad

    fixed = lambda shape: pl.BlockSpec(shape, lambda j, at: tuple(0 for _ in shape))
    return pl.pallas_call(
        kernel,
        out_shape=[jax.ShapeDtypeStruct((3, width), f32), jax.ShapeDtypeStruct((2, width), f32)],
        grid_spec=pltpu.PrefetchScalarGridSpec(
            num_scalar_prefetch=1,
            grid=(1,),
            in_specs=[
                fixed(arrived.shape),
                pl.BlockSpec((1, 2, width), lambda j, at: (at[0], 0, 0)),
                fixed((1, width)),
            ],
            out_specs=[fixed((3, width)), fixed((2, width))],
        ),
        compiler_params=params(8),
        name="combine_grads",
    )(where, arrived, stb, gain)


def weight_grad(own_l, other_l, own_r, other_r, terms=1):
    micro, padded, left = own_l.shape
    right = own_r.shape[2] // terms
    block = 512
    steps = right // block

    def kernel(ol, pl_, *rest):
        mine, others, out = rest[:terms], rest[terms:-1], rest[-1]
        contract = (((0,), (0,)), ((), ()))
        dot = lambda a, b: lax.dot_general(a, b, contract, preferred_element_type=f32)
        total = 0.0
        for m in range(micro):
            for k in range(terms):
                total += dot(ol[m], mine[k][m])
                total += dot(pl_[m], others[m * terms + k][...])
        out[...] = total.astype(bf16)

    def mine_at(k):
        return pl.BlockSpec((micro, padded, block), lambda j: (0, 0, j + k * steps))

    def other_at(k):
        return pl.BlockSpec((padded, block), lambda j: (0, j + k * steps))

    return pl.pallas_call(
        kernel,
        grid=(steps,),
        in_specs=[pl.BlockSpec(own_l.shape, lambda j: (0, 0, 0))] * 2
        + [mine_at(k) for k in range(terms)]
        + [other_at(k) for m in range(micro) for k in range(terms)],
        out_specs=pl.BlockSpec((left, block), lambda j: (0, j)),
        out_shape=jax.ShapeDtypeStruct((left, right), bf16),
        compiler_params=params(),
        name="weight_grad",
    )(own_l, other_l, *[own_r] * terms, *[r for r in other_r for _ in range(terms)])


def half_columns(x, count, core):
    width = x.shape[-1]
    part = width // count
    k = lax.broadcasted_iota(jnp.int32, (width, width // 2), 0)
    n = lax.broadcasted_iota(jnp.int32, (width, width // 2), 1)
    select = (k == (n // part) * (2 * part) + core * part + n % part).astype(bf16)
    return jnp.dot(x, select, preferred_element_type=f32).astype(bf16)


def local(images, cotangent, w_in, w_out, gain, shift):
    sections = lax.axis_size("section")
    replicas = lax.axis_size("dp")
    section = lax.axis_index("section")
    core = lax.axis_index("dp") % 2
    micro, rows_local, width = images.shape
    hidden = w_in.shape[2]
    rows = rows_local * replicas
    padded = -(-rows_local // 16) * 16
    ticks = micro + sections - 1
    up_route = [(i, i + 1) for i in range(sections - 1)]
    down_route = [(i + 1, i) for i in range(sections - 1)]
    swap_route = [(i, i ^ 1) for i in range(replicas)]

    def exchange(copies):
        return lax.all_to_all(copies, "dp", split_axis=0, concat_axis=0, tiled=True)

    def swap(x):
        return lax.ppermute(x, "dp", swap_route)

    def place(offset, edge, index):
        valid = (offset >= 0) & (offset < micro)
        slot = jnp.where(valid, offset, 2)
        return jnp.stack([slot, edge.astype(jnp.int32), jnp.int32(index)]).astype(jnp.int32)

    def forward_step(tick, state):
        where = place(tick - section, section == 0, min(tick, micro - 1))
        bufs, sent, part = forward(
            where, images, state["x"], stats_img, state["st"], gain, shift, w_in, w_out, state["bufs"], replicas, padded
        )
        state["bufs"] = bufs
        if tick + 1 < ticks:
            everyone = exchange(part)
            state["x"] = lax.ppermute(sent, "section", up_route)
            state["st"] = lax.ppermute(combine_stats(everyone, rows, rows_local), "section", up_route)

    grads = []

    def backward_step(tick, state, back):
        where = place(tick - (sections - 1 - section), section == sections - 1, min(tick, micro - 1))
        xb, stb, _, _, slb, outb = state["bufs"]
        bufs, sent, part = backward(
            where, cotangent, back["u"], back["fix"], gain, w_in, w_out, (xb, stb, slb, outb), back["bufs"], replicas, padded
        )
        back["bufs"] = bufs
        everyone = exchange(part)
        if tick + 1 < ticks:
            back["u"] = lax.ppermute(sent, "section", down_route)
        fix, sums = combine_grads(where, everyone, stb, gain, rows)
        grads.append((fix, sums))
        if tick + 1 < ticks:
            back["fix"] = lax.ppermute(fix, "section", down_route)

    stats_img = combine_stats(exchange(image_stats(images, replicas)), rows, rows_local)
    state = {
        "x": jnp.zeros((rows_local, width), bf16),
        "st": jnp.zeros((1, 2, width), f32),
        "bufs": [],
    }
    back = {
        "u": jnp.zeros((rows_local, width), bf16),
        "fix": jnp.zeros((3, width), f32),
        "bufs": [],
    }
    for tick in range(ticks - 1):
        forward_step(tick, state)
    backward_step(0, state, back)
    forward_step(ticks - 1, state)
    for tick in range(1, ticks - 1):
        backward_step(tick, state, back)

    affb, actb = state["bufs"][2][:micro], state["bufs"][3][:micro]
    own_aff, own_act = half_columns(affb, replicas, core), half_columns(actb, replicas, core)
    other_aff = swap(half_columns(affb, replicas, 1 - core))
    other_act = swap(half_columns(actb, replicas, 1 - core))
    other_up, other_gb = [swap(back["bufs"][0][0])], [swap(back["bufs"][1][0])]
    for tick in range(ticks - 1, ticks):
        backward_step(tick, state, back)
    upb, gbb, ub = back["bufs"]
    for m in range(1, micro):
        other_up.append(swap(upb[m]))
        other_gb.append(swap(gbb[m]))

    groups = [list(range(c, replicas, 2)) for c in range(2)]

    def reduced(part):
        blocks = part.reshape(replicas // 2, -1, part.shape[1])
        got = lax.all_to_all(blocks, "dp", split_axis=0, concat_axis=0, axis_index_groups=groups, tiled=True)
        return got.astype(f32).sum(axis=0)

    reduced_out = reduced(weight_grad(own_act, other_act, upb, other_up, 2))
    reduced_in = reduced(weight_grad(own_aff, other_aff, gbb, other_gb))

    fixes = jnp.stack([g[0] for g in grads])
    sums = jnp.stack([g[1] for g in grads])
    start = sections - 1 - section
    fixes = lax.dynamic_slice_in_dim(fixes, start, micro, 0)
    sums = lax.dynamic_slice_in_dim(sums, start, micro, 0).sum(axis=0)
    x = state["bufs"][0][:micro].astype(f32)
    in_grads = (ub[:micro] - fixes[:, 0:1] - fixes[:, 1:2] * (x - fixes[:, 2:3])).astype(bf16)
    return (
        state["bufs"][5][:micro][None],
        in_grads[None],
        reduced_in[None],
        reduced_out[None],
        sums[0:1],
        sums[1:2],
    )


def solution(mesh):
    placed = (
        P(None, "dp", None),
        P(None, "dp", None),
        P("section", None, None),
        P("section", None, None),
        P("section", None),
        P("section", None),
    )
    return jax.shard_map(
        local,
        mesh=mesh,
        in_specs=placed,
        out_specs=(
            P("section", None, "dp", None),
            P("section", None, "dp", None),
            P("section", "dp", None),
            P("section", "dp", None),
            P("section", None),
            P("section", None),
        ),
        check_vma=False,
    )
```

```python
import jax
import jax.numpy as jnp
from jax import lax
from jax.experimental import pallas as pl
from jax.experimental.pallas import tpu as pltpu
from jax.sharding import PartitionSpec as P

epsilon = 1e-05
gelu_scale = 0.7978845608028654
cubic_term = 0.044715
f32 = jnp.float32
bf16 = jnp.bfloat16


def gelu_parts(before):
    square = before * before
    inner = gelu_scale * (before + cubic_term * square * before)
    bend = jnp.tanh(inner)
    half = 0.5 * (1.0 + bend)
    value = before * half
    slope = half + 0.5 * before * (1.0 - bend * bend) * gelu_scale * (1.0 + 3.0 * cubic_term * square)
    return (value, slope)


def params(mib=59):
    return pltpu.CompilerParams(vmem_limit_bytes=mib * 1024 * 1024)


def row_mask(padded, rows):
    return lax.broadcasted_iota(jnp.int32, (padded, 1), 0) < rows


def moments(x, rows):
    total = jnp.sum(x, axis=0, keepdims=True)
    off = x - total / rows
    return total, jnp.sum(off * off, axis=0, keepdims=True)


def keep_padded(ref, x):
    rows = x.shape[0]
    whole = rows - rows % 8
    ref[whole:, :] = jnp.zeros((ref.shape[0] - whole, ref.shape[1]), ref.dtype)
    ref[:rows, :] = x


def fill_copies(ref, rows_of):
    for i, row in enumerate(rows_of):
        ref[:, i : i + 1, :] = jnp.broadcast_to(row[None], (ref.shape[0], 1, row.shape[1]))


def image_stats(images, copies):
    micro, rows, width = images.shape

    def kernel(x_ref, out_ref):
        parts = []
        for m in range(micro):
            parts += list(moments(x_ref[m].astype(f32), rows))
        fill_copies(out_ref, parts)

    return pl.pallas_call(
        kernel,
        grid=(1,),
        in_specs=[pl.BlockSpec((micro, rows, width), lambda i: (0, 0, 0))],
        out_specs=pl.BlockSpec((copies, 2 * micro, width), lambda i: (0, 0, 0)),
        out_shape=jax.ShapeDtypeStruct((copies, 2 * micro, width), f32),
        compiler_params=params(8),
        name="image_stats",
    )(images)


def combine_stats(arrived, rows, rows_local):
    _, twice, width = arrived.shape

    def kernel(a_ref, out_ref):
        for m in range(twice // 2):
            sums = a_ref[:, 2 * m, :]
            mean = jnp.sum(sums, axis=0, keepdims=True) / rows
            off = sums / rows_local - mean
            squares = jnp.sum(a_ref[:, 2 * m + 1, :], axis=0, keepdims=True)
            squares = squares + rows_local * jnp.sum(off * off, axis=0, keepdims=True)
            out_ref[m, 0:1, :] = mean
            out_ref[m, 1:2, :] = lax.rsqrt(squares / rows + epsilon)

    return pl.pallas_call(
        kernel,
        grid=(1,),
        in_specs=[pl.BlockSpec(arrived.shape, lambda i: (0, 0, 0))],
        out_specs=pl.BlockSpec((twice // 2, 2, width), lambda i: (0, 0, 0)),
        out_shape=jax.ShapeDtypeStruct((twice // 2, 2, width), f32),
        compiler_params=params(8),
        name="combine_stats",
    )(arrived)


small = pl.BlockSpec(memory_space=pltpu.SMEM)
whole = pl.BlockSpec(memory_space=pltpu.VMEM)
kept = pl.BlockSpec(memory_space=pltpu.HBM)
block = 512


def forward(tick, table, images, arrived, stats_img, stats_arr, gain, shift, w_in, w_out, bufs, copies, padded):
    _, rows, width = images.shape
    hidden = w_in.shape[2]
    cuts = [slice(j * block, (j + 1) * block) for j in range(hidden // block)]

    def kernel(at, img, arr, simg, sarr, g, sh, win, wout, *rest):
        rest = rest[len(bufs) :]
        xb, stb, affb, actb, slb, outb, send, part, in_s, x_s, st_s, aff_s, act_s, sl_s, w1, w2, sem_x, sem_1, sem_2, sem_o = rest
        came = arr.at[0] if len(arr.shape) == 3 else arr
        slot, first, micro_at = at[3 * tick], at[3 * tick + 1] == 1, at[3 * tick + 2]

        load_1 = [pltpu.make_async_copy(win.at[0, :, c], w1.at[:, c], sem_1.at[j]) for j, c in enumerate(cuts)]
        load_2 = [pltpu.make_async_copy(wout.at[0, c, :], w2.at[c, :], sem_2.at[j]) for j, c in enumerate(cuts)]

        @pl.when(first)
        def _():
            pltpu.make_async_copy(img.at[micro_at], in_s, sem_x).start()

        @pl.when(jnp.logical_not(first))
        def _():
            pltpu.make_async_copy(came, in_s, sem_x).start()

        for load in load_1 + load_2:
            load.start()
        pltpu.make_async_copy(came, in_s, sem_x).wait()
        stores = []

        def store(source, target):
            copy = pltpu.make_async_copy(source, target, sem_o.at[len(stores)])
            copy.start()
            stores.append(copy)

        st = jnp.where(first, simg[pl.ds(micro_at, 1)][0], sarr[0])
        st_s[...] = st
        store(in_s, xb.at[slot])
        store(st_s, stb.at[slot])
        keep_padded(x_s, in_s[...].astype(f32))
        affine = (x_s[...] - st[0:1]) * (st[1:2] * g[...]) + sh[...]
        affine = jnp.where(row_mask(padded, rows), affine, 0.0).astype(bf16)
        aff_s[...] = affine
        store(aff_s, affb.at[slot])

        def first_product(j):
            return jnp.dot(affine, w1[:, cuts[j]], preferred_element_type=f32)

        for load in load_1 + load_2:
            load.wait()
        before = first_product(0)
        for j, c in enumerate(cuts):
            coming = first_product(j + 1) if j + 1 < len(cuts) else None
            value, slope = gelu_parts(before)
            act_s[:, c] = value.astype(bf16)
            sl_s[:, c] = slope.astype(bf16)
            store(act_s.at[:, c], actb.at[slot, :, c])
            store(sl_s.at[:, c], slb.at[slot, :, c])
            before = coming
        grown = jnp.dot(act_s[...], w2[...], preferred_element_type=f32)
        output = (x_s[...] + grown)[:rows].astype(bf16)
        send[...] = output
        store(send, outb.at[slot])
        fill_copies(part, moments(output.astype(f32), rows))
        for copy in stores:
            copy.wait()

    out = pl.pallas_call(
        kernel,
        out_shape=[
            pltpu.HBM((3, rows, width), bf16),
            pltpu.HBM((3, 2, width), f32),
            pltpu.HBM((3, padded, width), bf16),
            pltpu.HBM((3, padded, hidden), bf16),
            pltpu.HBM((3, padded, hidden), bf16),
            pltpu.HBM((3, rows, width), bf16),
            jax.ShapeDtypeStruct((rows, width), bf16),
            jax.ShapeDtypeStruct((copies, 2, width), f32),
        ],
        in_specs=[small, kept, kept, whole, whole, whole, whole, kept, kept] + [kept] * len(bufs),
        out_specs=[kept] * 6 + [whole] * 2,
            scratch_shapes=[
                pltpu.VMEM((rows, width), bf16),
                pltpu.VMEM((padded, width), f32),
                pltpu.VMEM((2, width), f32),
                pltpu.VMEM((padded, width), bf16),
                pltpu.VMEM((padded, hidden), bf16),
                pltpu.VMEM((padded, hidden), bf16),
                pltpu.VMEM((width, hidden), bf16),
                pltpu.VMEM((hidden, width), bf16),
                pltpu.SemaphoreType.DMA(()),
                pltpu.SemaphoreType.DMA((len(cuts),)),
                pltpu.SemaphoreType.DMA((len(cuts),)),
                pltpu.SemaphoreType.DMA((4 + 2 * len(cuts),)),
            ],
        input_output_aliases={9 + i: i for i in range(len(bufs))},
        compiler_params=params(),
        name="section_forward",
    )(table, images, arrived, stats_img, stats_arr, gain, shift, w_in, w_out, *bufs)
    return list(out[:6]), out[6], out[7]


def backward(tick, table, cotangent, arrived, fix, gain, w_in_t, w_out_t, saved, bufs, copies, padded):
    _, rows, width = cotangent.shape
    hidden = saved[2].shape[2]
    cuts = [slice(j * block, (j + 1) * block) for j in range(hidden // block)]

    def kernel(at, cot, arr, fx, g, win, wout, xb, stb, slb, outb, *rest):
        rest = rest[len(bufs) :]
        upb, gbb, ub, send, part, in_s, own_s, x_s, st_s, sl_s, pad_s, up_s, keep_s, gb_s, u_s, w1, w2, sem_x, sem_k, sem_1, sem_2, sem_o = rest
        came = arr.at[0] if len(arr.shape) == 3 else arr
        slot, last, micro_at = at[3 * tick], at[3 * tick + 1] == 1, at[3 * tick + 2]

        load_1 = [pltpu.make_async_copy(win.at[0, :, c], w1.at[:, c], sem_1.at[j]) for j, c in enumerate(cuts)]
        load_2 = [pltpu.make_async_copy(wout.at[0, c, :], w2.at[c, :], sem_2.at[j]) for j, c in enumerate(cuts)]

        @pl.when(last)
        def _():
            pltpu.make_async_copy(cot.at[micro_at], in_s, sem_x).start()

        @pl.when(jnp.logical_not(last))
        def _():
            pltpu.make_async_copy(came, in_s, sem_x).start()

        loads = [
            pltpu.make_async_copy(source.at[slot], target, sem_k.at[n])
            for n, (source, target) in enumerate(((outb, own_s), (stb, st_s), (slb, sl_s), (xb, x_s)))
        ]
        for load in [loads[0], load_2[0], loads[2]] + load_2[1:] + loads[1:2] + loads[3:] + load_1:
            load.start()
        pltpu.make_async_copy(came, in_s, sem_x).wait()
        loads[0].wait()
        stores = []

        def store(source, target):
            copy = pltpu.make_async_copy(source, target, sem_o.at[len(stores)])
            copy.start()
            stores.append(copy)

        high = in_s[...].astype(f32)
        low = -fx[0:1] - fx[1:2] * (own_s[...].astype(f32) - fx[2:3])
        low = jnp.where(last, 0.0, low)
        keep_padded(pad_s, high)
        up_s[:padded] = pad_s[...].astype(bf16)
        keep_padded(pad_s, low)
        up_s[padded:] = pad_s[...].astype(bf16)
        u_s[...] = high + low
        keep_s[:, :width] = up_s[:padded]
        keep_s[:, width:] = up_s[padded:]
        store(keep_s, upb.at[slot])

        def first_product(j):
            both = lax.dot_general(up_s[...], w2[cuts[j], :], (((1,), (1,)), ((), ())), preferred_element_type=f32)
            return both[:padded] + both[padded:]

        for load in load_1 + load_2 + loads[1:]:
            load.wait()
        grad_active = first_product(0)
        for j, c in enumerate(cuts):
            coming = first_product(j + 1) if j + 1 < len(cuts) else None
            gb_s[:, c] = (grad_active * sl_s[:, c].astype(f32)).astype(bf16)
            store(gb_s.at[:, c], gbb.at[slot, :, c])
            grad_active = coming
        grad_affine = lax.dot_general(gb_s[...], w1[...], (((1,), (1,)), ((), ())), preferred_element_type=f32)[:rows]
        inverse = st_s[1:2, :]
        normed = (x_s[...].astype(f32) - st_s[0:1, :]) * inverse
        sum_grad = jnp.sum(grad_affine, axis=0, keepdims=True)
        sum_cross = jnp.sum(grad_affine * normed, axis=0, keepdims=True)
        fill_copies(part, (sum_grad, sum_cross))
        u = u_s[...] + inverse * g[...] * grad_affine
        u_s[...] = u
        send[...] = u.astype(bf16)
        store(u_s, ub.at[slot])
        for copy in stores:
            copy.wait()

    out = pl.pallas_call(
        kernel,
        out_shape=[
            pltpu.HBM((3, padded, 2 * width), bf16),
            pltpu.HBM((3, padded, hidden), bf16),
            pltpu.HBM((3, rows, width), f32),
            jax.ShapeDtypeStruct((rows, width), bf16),
            jax.ShapeDtypeStruct((copies, 2, width), f32),
        ],
        in_specs=[small, kept, kept, whole, whole, kept, kept] + [kept] * 4 + [kept] * len(bufs),
        out_specs=[kept] * 3 + [whole] * 2,
            scratch_shapes=[
                pltpu.VMEM((rows, width), bf16),
                pltpu.VMEM((rows, width), bf16),
                pltpu.VMEM((rows, width), bf16),
                pltpu.VMEM((2, width), f32),
                pltpu.VMEM((padded, hidden), bf16),
                pltpu.VMEM((padded, width), f32),
                pltpu.VMEM((2 * padded, width), bf16),
                pltpu.VMEM((padded, 2 * width), bf16),
                pltpu.VMEM((padded, hidden), bf16),
                pltpu.VMEM((rows, width), f32),
                pltpu.VMEM((width, hidden), bf16),
                pltpu.VMEM((hidden, width), bf16),
                pltpu.SemaphoreType.DMA(()),
                pltpu.SemaphoreType.DMA((4,)),
                pltpu.SemaphoreType.DMA((len(cuts),)),
                pltpu.SemaphoreType.DMA((len(cuts),)),
                pltpu.SemaphoreType.DMA((2 + len(cuts),)),
            ],
        input_output_aliases={11 + i: i for i in range(len(bufs))},
        compiler_params=params(),
        name="section_backward",
    )(table, cotangent, arrived, fix, gain, w_in_t, w_out_t, *saved, *bufs)
    return list(out[:3]), out[3], out[4]


def combine_grads(tick, table, arrived, stb, gain, rows):
    _, _, width = arrived.shape

    def kernel(at, a_ref, st, g, fix, sums):
        sum_grad = jnp.sum(a_ref[:, 0, :], axis=0, keepdims=True)
        sum_cross = jnp.sum(a_ref[:, 1, :], axis=0, keepdims=True)
        inverse = st[0, 1:2, :]
        scale = inverse * g[...]
        fix[0:1, :] = scale * (sum_grad / rows)
        fix[1:2, :] = scale * inverse * (sum_cross / rows)
        fix[2:3, :] = st[0, 0:1, :]
        sums[0:1, :] = sum_cross
        sums[1:2, :] = sum_grad

    fixed = lambda shape: pl.BlockSpec(shape, lambda j, at: tuple(0 for _ in shape))
    return pl.pallas_call(
        kernel,
        out_shape=[jax.ShapeDtypeStruct((3, width), f32), jax.ShapeDtypeStruct((2, width), f32)],
        grid_spec=pltpu.PrefetchScalarGridSpec(
            num_scalar_prefetch=1,
            grid=(1,),
            in_specs=[
                fixed(arrived.shape),
                pl.BlockSpec((1, 2, width), lambda j, at: (at[3 * tick], 0, 0)),
                fixed((1, width)),
            ],
            out_specs=[fixed((3, width)), fixed((2, width))],
        ),
        compiler_params=params(8),
        name="combine_grads",
    )(table, arrived, stb, gain)


def weight_grad(own_l, other_l, own_r, other_r, terms=1):
    micro, padded, left = own_l.shape
    right = own_r.shape[2] // terms
    block = 512
    steps = right // block

    def kernel(ol, pl_, *rest):
        mine, others, out = rest[:terms], rest[terms:-1], rest[-1]
        contract = (((0,), (0,)), ((), ()))
        dot = lambda a, b: lax.dot_general(a, b, contract, preferred_element_type=f32)
        total = 0.0
        for m in range(micro):
            for k in range(terms):
                total += dot(ol[m], mine[k][m])
                total += dot(pl_[m], others[m * terms + k][...])
        out[...] = total.astype(bf16)

    def mine_at(k):
        return pl.BlockSpec((micro, padded, block), lambda j: (0, 0, j + k * steps))

    def other_at(k):
        return pl.BlockSpec((padded, block), lambda j: (0, j + k * steps))

    return pl.pallas_call(
        kernel,
        grid=(steps,),
        in_specs=[pl.BlockSpec(own_l.shape, lambda j: (0, 0, 0))] * 2
        + [mine_at(k) for k in range(terms)]
        + [other_at(k) for _ in range(micro) for k in range(terms)],
        out_specs=pl.BlockSpec((left, block), lambda j: (0, j)),
        out_shape=jax.ShapeDtypeStruct((left, right), bf16),
        compiler_params=params(),
        name="weight_grad",
    )(own_l, other_l, *[own_r] * terms, *[r for r in other_r for _ in range(terms)])


def half_columns(x, count, core):
    width = x.shape[-1]
    part = width // count
    k = lax.broadcasted_iota(jnp.int32, (width, width // 2), 0)
    n = lax.broadcasted_iota(jnp.int32, (width, width // 2), 1)
    select = (k == (n // part) * (2 * part) + core * part + n % part).astype(bf16)
    return jnp.dot(x, select, preferred_element_type=f32).astype(bf16)


def local(images, cotangent, w_in, w_out, gain, shift):
    sections = lax.axis_size("section")
    replicas = lax.axis_size("dp")
    section = lax.axis_index("section")
    core = lax.axis_index("dp") % 2
    micro, rows_local, width = images.shape
    rows = rows_local * replicas
    padded = -(-rows_local // 16) * 16
    ticks = micro + sections - 1
    up_route = [(i, i + 1) for i in range(sections - 1)]
    down_route = [(i + 1, i) for i in range(sections - 1)]
    swap_route = [(i, i ^ 1) for i in range(replicas)]

    def exchange(copies):
        return lax.all_to_all(copies, "dp", split_axis=0, concat_axis=0, tiled=True)

    def swap(x):
        return lax.ppermute(x, "dp", swap_route)

    def place(offset, edge, index):
        valid = (offset >= 0) & (offset < micro)
        return [jnp.where(valid, offset, 2), edge.astype(jnp.int32), jnp.int32(index)]

    entries = []
    for tick in range(ticks):
        entries += place(tick - section, section == 0, min(tick, micro - 1))
    for tick in range(ticks):
        entries += place(tick - (sections - 1 - section), section == sections - 1, min(tick, micro - 1))
    table = jnp.stack([e.astype(jnp.int32) for e in entries])
    weights = (w_in, w_out)

    def forward_step(tick, state):
        bufs, sent, part = forward(
            tick, table, images, state["x"], stats_img, state["st"], gain, shift, *weights, state["bufs"], replicas, padded
        )
        state["bufs"] = bufs
        if tick + 1 < ticks:
            everyone = exchange(part)
            state["x"] = lax.ppermute(sent, "section", up_route)
            state["st"] = lax.ppermute(combine_stats(everyone, rows, rows_local), "section", up_route)

    grads = []

    def backward_step(tick, state, back):
        xb, stb, _, _, slb, outb = state["bufs"]
        bufs, sent, part = backward(
            ticks + tick, table, cotangent, back["u"], back["fix"], gain, *weights, (xb, stb, slb, outb), back["bufs"], replicas, padded
        )
        back["bufs"] = bufs
        everyone = exchange(part)
        if tick + 1 < ticks:
            back["u"] = lax.ppermute(sent, "section", down_route)
        fix, sums = combine_grads(ticks + tick, table, everyone, stb, gain, rows)
        grads.append((fix, sums))
        if tick + 1 < ticks:
            back["fix"] = lax.ppermute(fix, "section", down_route)

    stats_img = combine_stats(exchange(image_stats(images, replicas)), rows, rows_local)
    state = {"x": images, "st": stats_img, "bufs": []}
    back = {"u": cotangent, "fix": jnp.zeros((3, width), f32), "bufs": []}
    for tick in range(ticks - 1):
        forward_step(tick, state)
    backward_step(0, state, back)
    forward_step(ticks - 1, state)
    backward_step(1, state, back)
    affb, actb = state["bufs"][2][:micro], state["bufs"][3][:micro]
    own_aff = half_columns(affb, replicas, core)
    other_aff = half_columns(affb, replicas, 1 - core)
    other_act = half_columns(actb, replicas, 1 - core)
    backward_step(2, state, back)
    own_act = half_columns(actb, replicas, core)
    other_aff, other_act = swap(other_aff), swap(other_act)
    for tick in range(3, ticks - 1):
        backward_step(tick, state, back)
    other_up, other_gb = [swap(back["bufs"][0][0])], [swap(back["bufs"][1][0])]
    for tick in range(ticks - 1, ticks):
        backward_step(tick, state, back)
    upb, gbb, ub = back["bufs"]
    for m in range(1, micro):
        other_up.append(swap(upb[m]))
        other_gb.append(swap(gbb[m]))

    groups = [list(range(c, replicas, 2)) for c in range(2)]

    def reduced(part):
        blocks = part.reshape(replicas // 2, -1, part.shape[1])
        got = lax.all_to_all(blocks, "dp", split_axis=0, concat_axis=0, axis_index_groups=groups, tiled=True)
        return got.astype(f32).sum(axis=0)

    reduced_out = reduced(weight_grad(own_act, other_act, upb, other_up, 2))
    reduced_in = reduced(weight_grad(own_aff, other_aff, gbb, other_gb))

    fixes = jnp.stack([g[0] for g in grads])
    sums = jnp.stack([g[1] for g in grads])
    start = sections - 1 - section
    fixes = lax.dynamic_slice_in_dim(fixes, start, micro, 0)
    sums = lax.dynamic_slice_in_dim(sums, start, micro, 0).sum(axis=0)
    x = state["bufs"][0][:micro].astype(f32)
    in_grads = (ub[:micro] - fixes[:, 0:1] - fixes[:, 1:2] * (x - fixes[:, 2:3])).astype(bf16)
    return (
        state["bufs"][5][:micro][None],
        in_grads[None],
        reduced_in[None],
        reduced_out[None],
        sums[0:1],
        sums[1:2],
    )


def solution(mesh):
    placed = (
        P(None, "dp", None),
        P(None, "dp", None),
        P("section", None, None),
        P("section", None, None),
        P("section", None),
        P("section", None),
    )
    return jax.shard_map(
        local,
        mesh=mesh,
        in_specs=placed,
        out_specs=(
            P("section", None, "dp", None),
            P("section", None, "dp", None),
            P("section", "dp", None),
            P("section", "dp", None),
            P("section", None),
            P("section", None),
        ),
        check_vma=False,
    )
```

```python
import jax
import jax.numpy as jnp
from jax import lax
from jax.experimental import pallas as pl
from jax.experimental.pallas import tpu as pltpu
from jax.sharding import PartitionSpec as P

epsilon = 1e-05
gelu_scale = 0.7978845608028654
cubic_term = 0.044715
f32 = jnp.float32
bf16 = jnp.bfloat16


def gelu_parts(before):
    square = before * before
    inner = gelu_scale * (before + cubic_term * square * before)
    bend = jnp.tanh(inner)
    half = 0.5 * (1.0 + bend)
    value = before * half
    slope = half + 0.5 * before * (1.0 - bend * bend) * gelu_scale * (1.0 + 3.0 * cubic_term * square)
    return (value, slope)


def params(mib=59):
    return pltpu.CompilerParams(vmem_limit_bytes=mib * 1024 * 1024)


def row_mask(padded, rows):
    return lax.broadcasted_iota(jnp.int32, (padded, 1), 0) < rows


def moments(x, rows):
    total = jnp.sum(x, axis=0, keepdims=True)
    off = x - total / rows
    return total, jnp.sum(off * off, axis=0, keepdims=True)


def keep_padded(ref, x):
    rows = x.shape[0]
    whole = rows - rows % 8
    ref[whole:, :] = jnp.zeros((ref.shape[0] - whole, ref.shape[1]), ref.dtype)
    ref[:rows, :] = x


def fill_copies(ref, rows_of):
    for i, row in enumerate(rows_of):
        ref[:, i : i + 1, :] = jnp.broadcast_to(row[None], (ref.shape[0], 1, row.shape[1]))


def image_stats(images, copies):
    micro, rows, width = images.shape

    def kernel(x_ref, out_ref):
        parts = []
        for m in range(micro):
            parts += list(moments(x_ref[m].astype(f32), rows))
        fill_copies(out_ref, parts)

    return pl.pallas_call(
        kernel,
        grid=(1,),
        in_specs=[pl.BlockSpec((micro, rows, width), lambda i: (0, 0, 0))],
        out_specs=pl.BlockSpec((copies, 2 * micro, width), lambda i: (0, 0, 0)),
        out_shape=jax.ShapeDtypeStruct((copies, 2 * micro, width), f32),
        compiler_params=params(8),
        name="image_stats",
    )(images)


def combine_stats(arrived, rows, rows_local):
    _, twice, width = arrived.shape

    def kernel(a_ref, out_ref):
        for m in range(twice // 2):
            sums = a_ref[:, 2 * m, :]
            mean = jnp.sum(sums, axis=0, keepdims=True) / rows
            off = sums / rows_local - mean
            squares = jnp.sum(a_ref[:, 2 * m + 1, :], axis=0, keepdims=True)
            squares = squares + rows_local * jnp.sum(off * off, axis=0, keepdims=True)
            out_ref[m, 0:1, :] = mean
            out_ref[m, 1:2, :] = lax.rsqrt(squares / rows + epsilon)

    return pl.pallas_call(
        kernel,
        grid=(1,),
        in_specs=[pl.BlockSpec(arrived.shape, lambda i: (0, 0, 0))],
        out_specs=pl.BlockSpec((twice // 2, 2, width), lambda i: (0, 0, 0)),
        out_shape=jax.ShapeDtypeStruct((twice // 2, 2, width), f32),
        compiler_params=params(8),
        name="combine_stats",
    )(arrived)


small = pl.BlockSpec(memory_space=pltpu.SMEM)
whole = pl.BlockSpec(memory_space=pltpu.VMEM)
kept = pl.BlockSpec(memory_space=pltpu.HBM)
block = 512


def forward(turn, mine, arrived, stats, gain, shift, w_in, w_out, bufs, copies, rows, padded):
    micro, _, width = stats.shape
    loose = len(arrived.shape) == 3
    hidden = w_in.shape[2]
    tall = micro * padded
    cuts = [slice(j * block, (j + 1) * block) for j in range(hidden // block)]

    def kernel(at, arr, stats_ref, g, sh, win, wout, *rest):
        rest = rest[len(bufs) :]
        xb, stb, affb, actb, slb, outb, send, part = rest[:8]
        raw_s, in_s, x_s, aff_s, act_s, sl_s, w1, w2, sem_x, sem_w, sem_o = rest[8:]

        @pl.when(at[0] == turn)
        def _():
            loads = [
                pltpu.make_async_copy(win.at[0], w1, sem_w.at[0]),
                pltpu.make_async_copy(wout.at[0], w2, sem_w.at[1]),
            ]
            enter = pltpu.make_async_copy(arr, raw_s if loose else in_s, sem_x)
            enter.start()
            for load in loads:
                load.start()
            enter.wait()
            stores = []

            def store(source, target):
                copy = pltpu.make_async_copy(source, target, sem_o.at[len(stores)])
                copy.start()
                stores.append(copy)

            if loose:
                for m in range(micro):
                    keep_padded(x_s.at[pl.ds(m * padded, padded)], raw_s[m].astype(f32))
                in_s[...] = x_s[...].astype(bf16)
            else:
                x_s[...] = in_s[...].astype(f32)
            store(in_s, xb)
            store(stats_ref, stb)
            mask = row_mask(padded, rows)
            for m in range(micro):
                at_m = pl.ds(m * padded, padded)
                affine = (x_s[at_m] - stats_ref[m, 0:1]) * (stats_ref[m, 1:2] * g[...]) + sh[...]
                aff_s[at_m] = jnp.where(mask, affine, 0.0).astype(bf16)
            store(aff_s, affb)
            for load in loads:
                load.wait()

            def first_product(j):
                return jnp.dot(aff_s[...], w1[:, cuts[j]], preferred_element_type=f32)

            before = first_product(0)
            for j, c in enumerate(cuts):
                coming = first_product(j + 1) if j + 1 < len(cuts) else None
                value, slope = gelu_parts(before)
                act_s[:, c] = value.astype(bf16)
                sl_s[:, c] = slope.astype(bf16)
                store(act_s.at[:, c], actb.at[:, c])
                store(sl_s.at[:, c], slb.at[:, c])
                before = coming
            grown = jnp.dot(act_s[...], w2[...], preferred_element_type=f32)
            sums = []
            for m in range(micro):
                output = (x_s[pl.ds(m * padded, padded)] + grown[m * padded : (m + 1) * padded]).astype(bf16)
                send[pl.ds(m * padded, padded)] = output
                sums += list(moments(output[:rows].astype(f32), rows))
            store(send, outb)
            fill_copies(part, sums)
            for copy in stores:
                copy.wait()

    out = pl.pallas_call(
        kernel,
        out_shape=[
            pltpu.HBM((tall, width), bf16),
            pltpu.HBM((micro, 2, width), f32),
            pltpu.HBM((tall, width), bf16),
            pltpu.HBM((tall, hidden), bf16),
            pltpu.HBM((tall, hidden), bf16),
            pltpu.HBM((tall, width), bf16),
            jax.ShapeDtypeStruct((tall, width), bf16),
            jax.ShapeDtypeStruct((copies, 2 * micro, width), f32),
        ],
        in_specs=[small, kept, whole, whole, whole, kept, kept] + [kept] * len(bufs),
        out_specs=[kept] * 6 + [whole] * 2,
        scratch_shapes=[
            pltpu.VMEM((micro, rows, width), bf16),
            pltpu.VMEM((tall, width), bf16),
            pltpu.VMEM((tall, width), f32),
            pltpu.VMEM((tall, width), bf16),
            pltpu.VMEM((tall, hidden), bf16),
            pltpu.VMEM((tall, hidden), bf16),
            pltpu.VMEM((width, hidden), bf16),
            pltpu.VMEM((hidden, width), bf16),
            pltpu.SemaphoreType.DMA(()),
            pltpu.SemaphoreType.DMA((2,)),
            pltpu.SemaphoreType.DMA((4 + 2 * len(cuts),)),
        ],
        input_output_aliases={7 + i: i for i in range(len(bufs))},
        compiler_params=params(),
        name="section_forward",
    )(mine, arrived, stats, gain, shift, w_in, w_out, *bufs)
    return list(out[:6]), out[6], out[7]


def backward(turn, last, mine, arrived, fix, gain, w_in, w_out, saved, bufs, copies, rows, padded):
    micro, _, width = fix.shape
    loose = len(arrived.shape) == 3
    hidden = saved[2].shape[1]
    tall = micro * padded
    cuts = [slice(j * block, (j + 1) * block) for j in range(hidden // block)]
    contract = (((1,), (1,)), ((), ()))

    def kernel(at, arr, fx, g, win, wout, xb, stb, slb, outb, *rest):
        rest = rest[len(bufs) :]
        upb, gbb, ub, send, part = rest[:5]
        raw_s, in_s, own_s, x_s, st_s, sl_s, pad_s, up_s, keep_s, gb_s, u_s, w1, w2, sem_x, sem_k, sem_o = rest[5:]

        @pl.when(at[0] == turn)
        def _():
            pairs = ((wout.at[0], w2), (slb, sl_s), (win.at[0], w1), (xb, x_s), (stb, st_s))
            loads = [pltpu.make_async_copy(source, target, sem_k.at[n]) for n, (source, target) in enumerate(pairs)]
            enter = [pltpu.make_async_copy(arr, raw_s if loose else in_s, sem_x.at[0]), pltpu.make_async_copy(outb, own_s, sem_x.at[1])]
            for load in enter + loads:
                load.start()
            for load in enter:
                load.wait()
            stores = []

            def store(source, target):
                copy = pltpu.make_async_copy(source, target, sem_o.at[len(stores)])
                copy.start()
                stores.append(copy)

            mask = row_mask(padded, rows)
            for m in range(micro):
                at_m = pl.ds(m * padded, padded)
                if loose:
                    keep_padded(pad_s, raw_s[m].astype(f32))
                    high = pad_s[...]
                else:
                    high = in_s[at_m].astype(f32)
                if last:
                    low = jnp.zeros_like(high)
                else:
                    low = -fx[m, 0:1] - fx[m, 1:2] * (own_s[at_m].astype(f32) - fx[m, 2:3])
                    low = jnp.where(mask, low, 0.0)
                u_s[at_m] = high + low
                up_s[at_m] = high.astype(bf16)
                up_s[pl.ds(tall + m * padded, padded)] = low.astype(bf16)
            keep_s[:, :width] = up_s[:tall]
            keep_s[:, width:] = up_s[tall:]
            store(keep_s, upb)
            for load in loads:
                load.wait()

            def first_product(j):
                if last:
                    return lax.dot_general(up_s[:tall], w2[cuts[j], :], contract, preferred_element_type=f32)
                both = lax.dot_general(up_s[...], w2[cuts[j], :], contract, preferred_element_type=f32)
                return both[:tall] + both[tall:]

            grad_active = first_product(0)
            for j, c in enumerate(cuts):
                coming = first_product(j + 1) if j + 1 < len(cuts) else None
                gb_s[:, c] = (grad_active * sl_s[:, c].astype(f32)).astype(bf16)
                store(gb_s.at[:, c], gbb.at[:, c])
                grad_active = coming
            whole_grad = lax.dot_general(gb_s[...], w1[...], contract, preferred_element_type=f32)
            sums = []
            for m in range(micro):
                at_m = pl.ds(m * padded, padded)
                grad_affine = whole_grad[m * padded : (m + 1) * padded]
                inverse = st_s[m, 1:2, :]
                normed = (x_s[at_m].astype(f32) - st_s[m, 0:1, :]) * inverse
                sums.append(jnp.sum(grad_affine, axis=0, keepdims=True))
                sums.append(jnp.sum(grad_affine * normed, axis=0, keepdims=True))
                u = u_s[at_m] + inverse * g[...] * grad_affine
                u_s[at_m] = u
                send[at_m] = u.astype(bf16)
            store(u_s, ub)
            fill_copies(part, sums)
            for copy in stores:
                copy.wait()

    out = pl.pallas_call(
        kernel,
        out_shape=[
            pltpu.HBM((tall, 2 * width), bf16),
            pltpu.HBM((tall, hidden), bf16),
            pltpu.HBM((tall, width), f32),
            jax.ShapeDtypeStruct((tall, width), bf16),
            jax.ShapeDtypeStruct((copies, 2 * micro, width), f32),
        ],
        in_specs=[small, kept, whole, whole, kept, kept] + [kept] * 4 + [kept] * len(bufs),
        out_specs=[kept] * 3 + [whole] * 2,
        scratch_shapes=[
            pltpu.VMEM((micro, rows, width), bf16),
            pltpu.VMEM((tall, width), bf16),
            pltpu.VMEM((tall, width), bf16),
            pltpu.VMEM((tall, width), bf16),
            pltpu.VMEM((micro, 2, width), f32),
            pltpu.VMEM((tall, hidden), bf16),
            pltpu.VMEM((padded, width), f32),
            pltpu.VMEM((2 * tall, width), bf16),
            pltpu.VMEM((tall, 2 * width), bf16),
            pltpu.VMEM((tall, hidden), bf16),
            pltpu.VMEM((tall, width), f32),
            pltpu.VMEM((width, hidden), bf16),
            pltpu.VMEM((hidden, width), bf16),
            pltpu.SemaphoreType.DMA((2,)),
            pltpu.SemaphoreType.DMA((5,)),
            pltpu.SemaphoreType.DMA((2 + len(cuts),)),
        ],
        input_output_aliases={10 + i: i for i in range(len(bufs))},
        compiler_params=params(),
        name="section_backward",
    )(mine, arrived, fix, gain, w_in, w_out, *saved, *bufs)
    return list(out[:3]), out[3], out[4]


def combine_grads(arrived, stb, gain, rows):
    _, twice, width = arrived.shape
    micro = twice // 2

    def kernel(a_ref, st, g, fix, sums):
        cross_all, grad_all = 0.0, 0.0
        for m in range(micro):
            sum_grad = jnp.sum(a_ref[:, 2 * m, :], axis=0, keepdims=True)
            sum_cross = jnp.sum(a_ref[:, 2 * m + 1, :], axis=0, keepdims=True)
            inverse = st[m, 1:2, :]
            scale = inverse * g[...]
            fix[m, 0:1, :] = scale * (sum_grad / rows)
            fix[m, 1:2, :] = scale * inverse * (sum_cross / rows)
            fix[m, 2:3, :] = st[m, 0:1, :]
            cross_all, grad_all = cross_all + sum_cross, grad_all + sum_grad
        sums[0:1, :] = cross_all
        sums[1:2, :] = grad_all

    return pl.pallas_call(
        kernel,
        out_shape=[jax.ShapeDtypeStruct((micro, 3, width), f32), jax.ShapeDtypeStruct((2, width), f32)],
        in_specs=[whole, whole, whole],
        out_specs=[whole, whole],
        compiler_params=params(8),
        name="combine_grads",
    )(arrived, stb, gain)


def weight_grad(own_l, other_l, own_r, other_r, terms=1):
    tall, left = own_l.shape
    right = own_r.shape[1] // terms
    steps = 2
    cut = right // steps

    def kernel(ol, pl_, *rest):
        mine, others, out = rest[:terms], rest[terms : 2 * terms], rest[-1]
        contract = (((0,), (0,)), ((), ()))
        dot = lambda a, b: lax.dot_general(a[...], b[...], contract, preferred_element_type=f32)
        total = 0.0
        for k in range(terms):
            total += dot(ol, mine[k])
            total += dot(pl_, others[k])
        out[...] = total.astype(bf16)

    def part_at(k):
        return pl.BlockSpec((tall, cut), lambda j: (0, j + k * steps))

    return pl.pallas_call(
        kernel,
        grid=(steps,),
        in_specs=[pl.BlockSpec(own_l.shape, lambda j: (0, 0))] * 2 + [part_at(k) for k in range(terms)] * 2,
        out_specs=pl.BlockSpec((left, cut), lambda j: (0, j)),
        out_shape=jax.ShapeDtypeStruct((left, right), bf16),
        compiler_params=params(),
        name="weight_grad",
    )(own_l, other_l, *[own_r] * terms, *[other_r] * terms)


def half_columns(x, count, core):
    width = x.shape[-1]
    part = width // count
    k = lax.broadcasted_iota(jnp.int32, (width, width // 2), 0)
    n = lax.broadcasted_iota(jnp.int32, (width, width // 2), 1)
    select = (k == (n // part) * (2 * part) + core * part + n % part).astype(bf16)
    return jnp.dot(x, select, preferred_element_type=f32).astype(bf16)


def local(images, cotangent, w_in, w_out, gain, shift):
    sections = lax.axis_size("section")
    replicas = lax.axis_size("dp")
    section = lax.axis_index("section")
    core = lax.axis_index("dp") % 2
    micro, rows_local, width = images.shape
    rows = rows_local * replicas
    padded = -(-rows_local // 16) * 16
    up_route = [(i, i + 1) for i in range(sections - 1)]
    down_route = [(i + 1, i) for i in range(sections - 1)]
    swap_route = [(i, i ^ 1) for i in range(replicas)]
    mine = section.astype(jnp.int32).reshape(1)

    def exchange(copies):
        return lax.all_to_all(copies, "dp", split_axis=0, concat_axis=0, tiled=True)

    def swap(x):
        return lax.ppermute(x, "dp", swap_route)

    stats = combine_stats(exchange(image_stats(images, replicas)), rows, rows_local)
    x, bufs = images, []
    for tick in range(sections):
        bufs, sent, part = forward(tick, mine, x, stats, gain, shift, w_in, w_out, bufs, replicas, rows_local, padded)
        if tick + 1 < sections:
            everyone = exchange(part)
            x = lax.ppermute(sent, "section", up_route)
            stats = lax.ppermute(combine_stats(everyone, rows, rows_local), "section", up_route)
    xb, stb, affb, actb, slb, outb = bufs

    u, fix, bufs, grads = cotangent, jnp.zeros((micro, 3, width), f32), [], []
    for tick in range(sections):
        turn = sections - 1 - tick
        bufs, sent, part = backward(
            turn, tick == 0, mine, u, fix, gain, w_in, w_out, (xb, stb, slb, outb), bufs, replicas, rows_local, padded
        )
        everyone = exchange(part)
        if tick + 1 < sections:
            u = lax.ppermute(sent, "section", down_route)
        fix, sums = combine_grads(everyone, stb, gain, rows)
        grads.append((fix, sums))
        if tick + 1 < sections:
            fix = lax.ppermute(fix, "section", down_route)
        if tick == 0:
            own_aff = half_columns(affb, replicas, core)
            other_aff = half_columns(affb, replicas, 1 - core)
            other_act = half_columns(actb, replicas, 1 - core)
        if tick == 1:
            own_act = half_columns(actb, replicas, core)
            other_aff, other_act = swap(other_aff), swap(other_act)
    upb, gbb, ub = bufs

    groups = [list(range(c, replicas, 2)) for c in range(2)]

    def reduced(part):
        blocks = part.reshape(replicas // 2, -1, part.shape[1])
        got = lax.all_to_all(blocks, "dp", split_axis=0, concat_axis=0, axis_index_groups=groups, tiled=True)
        return got.astype(f32).sum(axis=0)

    reduced_out = reduced(weight_grad(own_act, other_act, upb, swap(upb), 2))
    reduced_in = reduced(weight_grad(own_aff, other_aff, gbb, swap(gbb)))

    fixes, sums = grads[-1]
    for tick in range(sections - 1):
        own = section == sections - 1 - tick
        fixes = jnp.where(own, grads[tick][0], fixes)
        sums = jnp.where(own, grads[tick][1], sums)

    def per_micro(t):
        return t.reshape(micro, padded, width)[:, :rows_local]

    x = per_micro(xb).astype(f32)
    in_grads = (per_micro(ub) - fixes[:, 0:1] - fixes[:, 1:2] * (x - fixes[:, 2:3])).astype(bf16)
    return (
        per_micro(outb)[None],
        in_grads[None],
        reduced_in[None],
        reduced_out[None],
        sums[0:1],
        sums[1:2],
    )


def solution(mesh):
    placed = (
        P(None, "dp", None),
        P(None, "dp", None),
        P("section", None, None),
        P("section", None, None),
        P("section", None),
        P("section", None),
    )
    return jax.shard_map(
        local,
        mesh=mesh,
        in_specs=placed,
        out_specs=(
            P("section", None, "dp", None),
            P("section", None, "dp", None),
            P("section", "dp", None),
            P("section", "dp", None),
            P("section", None),
            P("section", None),
        ),
        check_vma=False,
    )
```

```python
import jax
import jax.numpy as jnp
from jax import lax
from jax.experimental import pallas as pl
from jax.experimental.pallas import tpu as pltpu
from jax.sharding import PartitionSpec as P

epsilon = 1e-05
gelu_scale = 0.7978845608028654
cubic_term = 0.044715
f32 = jnp.float32
bf16 = jnp.bfloat16


def gelu_parts(before):
    square = before * before
    inner = gelu_scale * (before + cubic_term * square * before)
    bend = jnp.tanh(inner)
    half = 0.5 * (1.0 + bend)
    value = before * half
    slope = half + 0.5 * before * (1.0 - bend * bend) * gelu_scale * (1.0 + 3.0 * cubic_term * square)
    return (value, slope)


def params(mib=59):
    return pltpu.CompilerParams(vmem_limit_bytes=mib * 1024 * 1024)


def row_mask(padded, rows):
    return lax.broadcasted_iota(jnp.int32, (padded, 1), 0) < rows


def moments(x, rows):
    total = jnp.sum(x, axis=0, keepdims=True)
    off = x - total / rows
    return total, jnp.sum(off * off, axis=0, keepdims=True)


def keep_padded(ref, x):
    rows = x.shape[0]
    whole = rows - rows % 8
    ref[whole:, :] = jnp.zeros((ref.shape[0] - whole, ref.shape[1]), ref.dtype)
    ref[:rows, :] = x


def fill_copies(ref, rows_of):
    for i, row in enumerate(rows_of):
        ref[:, i : i + 1, :] = jnp.broadcast_to(row[None], (ref.shape[0], 1, row.shape[1]))


def image_stats(images, copies):
    micro, rows, width = images.shape

    def kernel(x_ref, out_ref):
        parts = []
        for m in range(micro):
            parts += list(moments(x_ref[m].astype(f32), rows))
        fill_copies(out_ref, parts)

    return pl.pallas_call(
        kernel,
        grid=(1,),
        in_specs=[pl.BlockSpec((micro, rows, width), lambda i: (0, 0, 0))],
        out_specs=pl.BlockSpec((copies, 2 * micro, width), lambda i: (0, 0, 0)),
        out_shape=jax.ShapeDtypeStruct((copies, 2 * micro, width), f32),
        compiler_params=params(8),
        name="image_stats",
    )(images)


def combine_stats(arrived, rows, rows_local):
    _, twice, width = arrived.shape

    def kernel(a_ref, out_ref):
        for m in range(twice // 2):
            sums = a_ref[:, 2 * m, :]
            mean = jnp.sum(sums, axis=0, keepdims=True) / rows
            off = sums / rows_local - mean
            squares = jnp.sum(a_ref[:, 2 * m + 1, :], axis=0, keepdims=True)
            squares = squares + rows_local * jnp.sum(off * off, axis=0, keepdims=True)
            out_ref[m, 0:1, :] = mean
            out_ref[m, 1:2, :] = lax.rsqrt(squares / rows + epsilon)

    return pl.pallas_call(
        kernel,
        grid=(1,),
        in_specs=[pl.BlockSpec(arrived.shape, lambda i: (0, 0, 0))],
        out_specs=pl.BlockSpec((twice // 2, 2, width), lambda i: (0, 0, 0)),
        out_shape=jax.ShapeDtypeStruct((twice // 2, 2, width), f32),
        compiler_params=params(8),
        name="combine_stats",
    )(arrived)


small = pl.BlockSpec(memory_space=pltpu.SMEM)
whole = pl.BlockSpec(memory_space=pltpu.VMEM)
kept = pl.BlockSpec(memory_space=pltpu.HBM)
block = 512


def forward(tick, table, images, arrived, stats_img, stats_arr, gain, shift, w_in, w_out, bufs, copies, padded):
    _, rows, width = images.shape
    hidden = w_in.shape[2]
    cuts = [slice(j * block, (j + 1) * block) for j in range(hidden // block)]

    def kernel(at, img, arr, simg, sarr, g, sh, w1, w2, *rest):
        rest = rest[len(bufs) :]
        xb, stb, affb, actb, slb, outb, send, part, in_s, x_s, st_s, aff_s, act_s, sl_s, sem_x, sem_o = rest
        came = arr.at[0] if len(arr.shape) == 3 else arr
        slot, first, micro_at = at[3 * tick], at[3 * tick + 1] == 1, at[3 * tick + 2]


        @pl.when(first)
        def _():
            pltpu.make_async_copy(img.at[micro_at], in_s, sem_x).start()

        @pl.when(jnp.logical_not(first))
        def _():
            pltpu.make_async_copy(came, in_s, sem_x).start()

        pltpu.make_async_copy(came, in_s, sem_x).wait()
        stores = []

        def store(source, target):
            copy = pltpu.make_async_copy(source, target, sem_o.at[len(stores)])
            copy.start()
            stores.append(copy)

        st = jnp.where(first, simg[pl.ds(micro_at, 1)][0], sarr[0])
        st_s[...] = st
        store(in_s, xb.at[slot])
        store(st_s, stb.at[slot])
        keep_padded(x_s, in_s[...].astype(f32))
        affine = (x_s[...] - st[0:1]) * (st[1:2] * g[...]) + sh[...]
        affine = jnp.where(row_mask(padded, rows), affine, 0.0).astype(bf16)
        aff_s[...] = affine
        store(aff_s, affb.at[slot])

        def first_product(j):
            return jnp.dot(affine, w1[0, :, cuts[j]], preferred_element_type=f32)

        before = first_product(0)
        for j, c in enumerate(cuts):
            coming = first_product(j + 1) if j + 1 < len(cuts) else None
            value, slope = gelu_parts(before)
            act_s[:, c] = value.astype(bf16)
            sl_s[:, c] = slope.astype(bf16)
            store(act_s.at[:, c], actb.at[slot, :, c])
            store(sl_s.at[:, c], slb.at[slot, :, c])
            before = coming
        grown = jnp.dot(act_s[...], w2[0], preferred_element_type=f32)
        output = (x_s[...] + grown)[:rows].astype(bf16)
        send[...] = output
        store(send, outb.at[slot])
        fill_copies(part, moments(output.astype(f32), rows))
        for copy in stores:
            copy.wait()

    out = pl.pallas_call(
        kernel,
        out_shape=[
            pltpu.HBM((3, rows, width), bf16),
            pltpu.HBM((3, 2, width), f32),
            pltpu.HBM((3, padded, width), bf16),
            pltpu.HBM((3, padded, hidden), bf16),
            pltpu.HBM((3, padded, hidden), bf16),
            pltpu.HBM((3, rows, width), bf16),
            pltpu.HBM((rows, width), bf16),
            pltpu.HBM((copies, 2, width), f32),
        ],
        in_specs=[small, kept, kept, whole, whole, whole, whole, whole, whole] + [kept] * len(bufs),
        out_specs=[kept] * 6 + [whole] * 2,
            scratch_shapes=[
                pltpu.VMEM((rows, width), bf16),
                pltpu.VMEM((padded, width), f32),
                pltpu.VMEM((2, width), f32),
                pltpu.VMEM((padded, width), bf16),
                pltpu.VMEM((padded, hidden), bf16),
                pltpu.VMEM((padded, hidden), bf16),
                pltpu.SemaphoreType.DMA(()),
                pltpu.SemaphoreType.DMA((4 + 2 * len(cuts),)),
            ],
        input_output_aliases={9 + i: i for i in range(len(bufs))},
        compiler_params=params(24),
        name="section_forward",
    )(table, images, arrived, stats_img, stats_arr, gain, shift, w_in, w_out, *bufs)
    return list(out[:6]), out[6], out[7]


def backward(tick, table, cotangent, arrived, fix, gain, w_in_t, w_out_t, saved, bufs, copies, padded):
    _, rows, width = cotangent.shape
    hidden = saved[2].shape[2]
    fresh = fix is gain
    cuts = [slice(j * block, (j + 1) * block) for j in range(hidden // block)]

    def kernel(at, cot, arr, fx, g, win, wout, xb, stb, slb, outb, *rest):
        rest = rest[len(bufs) :]
        upb, gbb, ub, send, part, in_s, own_s, x_s, st_s, sl_s, pad_s, up_s, keep_s, gb_s, u_s, w1, w2, sem_x, sem_k, sem_1, sem_2, sem_o = rest
        came = arr.at[0] if len(arr.shape) == 3 else arr
        slot, last, micro_at = at[3 * tick], at[3 * tick + 1] == 1, at[3 * tick + 2]

        load_1 = [pltpu.make_async_copy(win.at[0, :, c], w1.at[:, c], sem_1.at[j]) for j, c in enumerate(cuts)]
        load_2 = [pltpu.make_async_copy(wout.at[0, c, :], w2.at[c, :], sem_2.at[j]) for j, c in enumerate(cuts)]

        @pl.when(last)
        def _():
            pltpu.make_async_copy(cot.at[micro_at], in_s, sem_x).start()

        @pl.when(jnp.logical_not(last))
        def _():
            pltpu.make_async_copy(came, in_s, sem_x).start()

        loads = [
            pltpu.make_async_copy(source.at[slot], target, sem_k.at[n])
            for n, (source, target) in enumerate(((outb, own_s), (stb, st_s), (slb, sl_s), (xb, x_s)))
        ]
        for load in [loads[0], load_2[0], loads[2]] + load_2[1:] + loads[1:2] + loads[3:] + load_1:
            load.start()
        pltpu.make_async_copy(came, in_s, sem_x).wait()
        loads[0].wait()
        stores = []

        def store(source, target):
            copy = pltpu.make_async_copy(source, target, sem_o.at[len(stores)])
            copy.start()
            stores.append(copy)

        high = in_s[...].astype(f32)
        if fresh:
            low = jnp.zeros_like(high)
        else:
            low = -fx[0:1] - fx[1:2] * (own_s[...].astype(f32) - fx[2:3])
            low = jnp.where(last, 0.0, low)
        keep_padded(pad_s, high)
        up_s[:padded] = pad_s[...].astype(bf16)
        keep_padded(pad_s, low)
        up_s[padded:] = pad_s[...].astype(bf16)
        u_s[...] = high + low
        keep_s[:, :width] = up_s[:padded]
        keep_s[:, width:] = up_s[padded:]
        store(keep_s, upb.at[slot])

        def first_product(j):
            both = lax.dot_general(up_s[...], w2[cuts[j], :], (((1,), (1,)), ((), ())), preferred_element_type=f32)
            return both[:padded] + both[padded:]

        for load in load_1 + load_2 + loads[1:]:
            load.wait()
        grad_active = first_product(0)
        for j, c in enumerate(cuts):
            coming = first_product(j + 1) if j + 1 < len(cuts) else None
            gb_s[:, c] = (grad_active * sl_s[:, c].astype(f32)).astype(bf16)
            store(gb_s.at[:, c], gbb.at[slot, :, c])
            grad_active = coming
        grad_affine = lax.dot_general(gb_s[...], w1[...], (((1,), (1,)), ((), ())), preferred_element_type=f32)[:rows]
        inverse = st_s[1:2, :]
        normed = (x_s[...].astype(f32) - st_s[0:1, :]) * inverse
        sum_grad = jnp.sum(grad_affine, axis=0, keepdims=True)
        sum_cross = jnp.sum(grad_affine * normed, axis=0, keepdims=True)
        fill_copies(part, (sum_grad, sum_cross))
        u = u_s[...] + inverse * g[...] * grad_affine
        u_s[...] = u
        send[...] = u.astype(bf16)
        store(u_s, ub.at[slot])
        for copy in stores:
            copy.wait()

    out = pl.pallas_call(
        kernel,
        out_shape=[
            pltpu.HBM((3, padded, 2 * width), bf16),
            pltpu.HBM((3, padded, hidden), bf16),
            pltpu.HBM((3, rows, width), f32),
            jax.ShapeDtypeStruct((rows, width), bf16),
            jax.ShapeDtypeStruct((copies, 2, width), f32),
        ],
        in_specs=[small, kept, kept, whole, whole, kept, kept] + [kept] * 4 + [kept] * len(bufs),
        out_specs=[kept] * 3 + [whole] * 2,
            scratch_shapes=[
                pltpu.VMEM((rows, width), bf16),
                pltpu.VMEM((rows, width), bf16),
                pltpu.VMEM((rows, width), bf16),
                pltpu.VMEM((2, width), f32),
                pltpu.VMEM((padded, hidden), bf16),
                pltpu.VMEM((padded, width), f32),
                pltpu.VMEM((2 * padded, width), bf16),
                pltpu.VMEM((padded, 2 * width), bf16),
                pltpu.VMEM((padded, hidden), bf16),
                pltpu.VMEM((rows, width), f32),
                pltpu.VMEM((width, hidden), bf16),
                pltpu.VMEM((hidden, width), bf16),
                pltpu.SemaphoreType.DMA(()),
                pltpu.SemaphoreType.DMA((4,)),
                pltpu.SemaphoreType.DMA((len(cuts),)),
                pltpu.SemaphoreType.DMA((len(cuts),)),
                pltpu.SemaphoreType.DMA((2 + len(cuts),)),
            ],
        input_output_aliases={11 + i: i for i in range(len(bufs))},
        compiler_params=params(),
        name="section_backward",
    )(table, cotangent, arrived, fix, gain, w_in_t, w_out_t, *saved, *bufs)
    return list(out[:3]), out[3], out[4]


def combine_grads(tick, table, arrived, stb, gain, rows):
    _, _, width = arrived.shape

    def kernel(at, a_ref, st, g, fix, sums):
        sum_grad = jnp.sum(a_ref[:, 0, :], axis=0, keepdims=True)
        sum_cross = jnp.sum(a_ref[:, 1, :], axis=0, keepdims=True)
        inverse = st[0, 1:2, :]
        scale = inverse * g[...]
        fix[0:1, :] = scale * (sum_grad / rows)
        fix[1:2, :] = scale * inverse * (sum_cross / rows)
        fix[2:3, :] = st[0, 0:1, :]
        sums[0:1, :] = sum_cross
        sums[1:2, :] = sum_grad

    fixed = lambda shape: pl.BlockSpec(shape, lambda j, at: tuple(0 for _ in shape))
    return pl.pallas_call(
        kernel,
        out_shape=[jax.ShapeDtypeStruct((3, width), f32), jax.ShapeDtypeStruct((2, width), f32)],
        grid_spec=pltpu.PrefetchScalarGridSpec(
            num_scalar_prefetch=1,
            grid=(1,),
            in_specs=[
                fixed(arrived.shape),
                pl.BlockSpec((1, 2, width), lambda j, at: (at[3 * tick], 0, 0)),
                fixed((1, width)),
            ],
            out_specs=[fixed((3, width)), fixed((2, width))],
        ),
        compiler_params=params(8),
        name="combine_grads",
    )(table, arrived, stb, gain)


def weight_grad(own_l, other_l, own_r, other_r, terms=1):
    micro, padded, left = own_l.shape
    right = own_r.shape[2] // terms
    block = 512
    steps = right // block

    def kernel(ol, pl_, *rest):
        mine, others, out = rest[:terms], rest[terms:-1], rest[-1]
        contract = (((0,), (0,)), ((), ()))
        dot = lambda a, b: lax.dot_general(a, b, contract, preferred_element_type=f32)
        total = 0.0
        for m in range(micro):
            for k in range(terms):
                total += dot(ol[m], mine[k][m])
                total += dot(pl_[m], others[m * terms + k][...])
        out[...] = total.astype(bf16)

    def mine_at(k):
        return pl.BlockSpec((micro, padded, block), lambda j: (0, 0, j + k * steps))

    def other_at(k):
        return pl.BlockSpec((padded, block), lambda j: (0, j + k * steps))

    return pl.pallas_call(
        kernel,
        grid=(steps,),
        in_specs=[pl.BlockSpec(own_l.shape, lambda j: (0, 0, 0))] * 2
        + [mine_at(k) for k in range(terms)]
        + [other_at(k) for _ in range(micro) for k in range(terms)],
        out_specs=pl.BlockSpec((left, block), lambda j: (0, j)),
        out_shape=jax.ShapeDtypeStruct((left, right), bf16),
        compiler_params=params(),
        name="weight_grad",
    )(own_l, other_l, *[own_r] * terms, *[r for r in other_r for _ in range(terms)])


def half_columns(x, count, core):
    width = x.shape[-1]
    part = width // count
    k = lax.broadcasted_iota(jnp.int32, (width, width // 2), 0)
    n = lax.broadcasted_iota(jnp.int32, (width, width // 2), 1)
    select = (k == (n // part) * (2 * part) + core * part + n % part).astype(bf16)
    return jnp.dot(x, select, preferred_element_type=f32).astype(bf16)


def local(images, cotangent, w_in, w_out, gain, shift):
    sections = lax.axis_size("section")
    replicas = lax.axis_size("dp")
    section = lax.axis_index("section")
    core = lax.axis_index("dp") % 2
    micro, rows_local, _ = images.shape
    rows = rows_local * replicas
    padded = -(-rows_local // 16) * 16
    ticks = micro + sections - 1
    up_route = [(i, i + 1) for i in range(sections - 1)]
    down_route = [(i + 1, i) for i in range(sections - 1)]
    swap_route = [(i, i ^ 1) for i in range(replicas)]

    def exchange(copies):
        return lax.all_to_all(copies, "dp", split_axis=0, concat_axis=0, tiled=True)

    def swap(x):
        return lax.ppermute(x, "dp", swap_route)

    def place(offset, edge, index):
        valid = (offset >= 0) & (offset < micro)
        return [jnp.where(valid, offset, 2), edge.astype(jnp.int32), jnp.int32(index)]

    entries = []
    for tick in range(ticks):
        entries += place(tick - section, section == 0, min(tick, micro - 1))
    for tick in range(ticks):
        entries += place(tick - (sections - 1 - section), section == sections - 1, min(tick, micro - 1))
    table = jnp.stack([e.astype(jnp.int32) for e in entries])
    weights = (w_in, w_out)

    def forward_step(tick, state):
        bufs, sent, part = forward(
            tick, table, images, state["x"], stats_img, state["st"], gain, shift, *weights, state["bufs"], replicas, padded
        )
        state["bufs"] = bufs
        if tick + 1 < ticks:
            everyone = exchange(part)
            state["x"] = lax.ppermute(sent, "section", up_route)
            state["st"] = lax.ppermute(combine_stats(everyone, rows, rows_local), "section", up_route)

    grads = []

    def backward_step(tick, state, back):
        xb, stb, _, _, slb, outb = state["bufs"]
        bufs, sent, part = backward(
            ticks + tick, table, cotangent, back["u"], back["fix"], gain, *weights, (xb, stb, slb, outb), back["bufs"], replicas, padded
        )
        back["bufs"] = bufs
        everyone = exchange(part)
        if tick + 1 < ticks:
            back["u"] = lax.ppermute(sent, "section", down_route)
        fix, sums = combine_grads(ticks + tick, table, everyone, stb, gain, rows)
        grads.append((fix, sums))
        if tick + 1 < ticks:
            back["fix"] = lax.ppermute(fix, "section", down_route)

    stats_img = combine_stats(exchange(image_stats(images, replicas)), rows, rows_local)
    state = {"x": images, "st": stats_img, "bufs": []}
    back = {"u": cotangent, "fix": gain, "bufs": []}
    for tick in range(ticks - 1):
        forward_step(tick, state)
    backward_step(0, state, back)
    forward_step(ticks - 1, state)
    backward_step(1, state, back)
    affb, actb = state["bufs"][2][:micro], state["bufs"][3][:micro]
    own_aff = half_columns(affb, replicas, core)
    other_aff = half_columns(affb, replicas, 1 - core)
    other_act = half_columns(actb, replicas, 1 - core)
    backward_step(2, state, back)
    own_act = half_columns(actb, replicas, core)
    other_aff, other_act = swap(other_aff), swap(other_act)
    for tick in range(3, ticks - 1):
        backward_step(tick, state, back)
    other_up, other_gb = [swap(back["bufs"][0][0])], [swap(back["bufs"][1][0])]
    for tick in range(ticks - 1, ticks):
        backward_step(tick, state, back)
    upb, gbb, ub = back["bufs"]
    for m in range(1, micro):
        other_up.append(swap(upb[m]))
        other_gb.append(swap(gbb[m]))

    groups = [list(range(c, replicas, 2)) for c in range(2)]

    def reduced(part):
        blocks = part.reshape(replicas // 2, -1, part.shape[1])
        got = lax.all_to_all(blocks, "dp", split_axis=0, concat_axis=0, axis_index_groups=groups, tiled=True)
        return got.astype(f32).sum(axis=0)

    reduced_out = reduced(weight_grad(own_act, other_act, upb, other_up, 2))
    reduced_in = reduced(weight_grad(own_aff, other_aff, gbb, other_gb))

    fixes = jnp.stack([g[0] for g in grads])
    sums = jnp.stack([g[1] for g in grads])
    start = sections - 1 - section
    fixes = lax.dynamic_slice_in_dim(fixes, start, micro, 0)
    sums = lax.dynamic_slice_in_dim(sums, start, micro, 0).sum(axis=0)
    x = state["bufs"][0][:micro].astype(f32)
    in_grads = (ub[:micro] - fixes[:, 0:1] - fixes[:, 1:2] * (x - fixes[:, 2:3])).astype(bf16)
    return (
        state["bufs"][5][:micro][None],
        in_grads[None],
        reduced_in[None],
        reduced_out[None],
        sums[0:1],
        sums[1:2],
    )


def solution(mesh):
    placed = (
        P(None, "dp", None),
        P(None, "dp", None),
        P("section", None, None),
        P("section", None, None),
        P("section", None),
        P("section", None),
    )
    return jax.shard_map(
        local,
        mesh=mesh,
        in_specs=placed,
        out_specs=(
            P("section", None, "dp", None),
            P("section", None, "dp", None),
            P("section", "dp", None),
            P("section", "dp", None),
            P("section", None),
            P("section", None),
        ),
        check_vma=False,
    )
```

```python
import jax
import jax.numpy as jnp
from jax import lax
from jax.experimental import pallas as pl
from jax.experimental.pallas import tpu as pltpu
from jax.sharding import PartitionSpec as P

epsilon = 1e-05
gelu_scale = 0.7978845608028654
cubic_term = 0.044715
f32 = jnp.float32
bf16 = jnp.bfloat16


def gelu_parts(before):
    square = before * before
    inner = gelu_scale * (before + cubic_term * square * before)
    bend = jnp.tanh(inner)
    half = 0.5 * (1.0 + bend)
    value = before * half
    slope = half + 0.5 * before * (1.0 - bend * bend) * gelu_scale * (1.0 + 3.0 * cubic_term * square)
    return (value, slope)


def params(mib=59):
    return pltpu.CompilerParams(vmem_limit_bytes=mib * 1024 * 1024)


def row_mask(padded, rows):
    return lax.broadcasted_iota(jnp.int32, (padded, 1), 0) < rows


def moments(x, rows):
    total = jnp.sum(x, axis=0, keepdims=True)
    off = x - total / rows
    return total, jnp.sum(off * off, axis=0, keepdims=True)


def keep_padded(ref, x):
    rows = x.shape[0]
    whole = rows - rows % 8
    ref[whole:, :] = jnp.zeros((ref.shape[0] - whole, ref.shape[1]), ref.dtype)
    ref[:rows, :] = x


def fill_copies(ref, rows_of):
    for i, row in enumerate(rows_of):
        ref[:, i : i + 1, :] = jnp.broadcast_to(row[None], (ref.shape[0], 1, row.shape[1]))


def image_stats(images, copies):
    micro, rows, width = images.shape

    def kernel(x_ref, out_ref):
        parts = []
        for m in range(micro):
            parts += list(moments(x_ref[m].astype(f32), rows))
        fill_copies(out_ref, parts)

    return pl.pallas_call(
        kernel,
        grid=(1,),
        in_specs=[pl.BlockSpec((micro, rows, width), lambda i: (0, 0, 0))],
        out_specs=pl.BlockSpec((copies, 2 * micro, width), lambda i: (0, 0, 0)),
        out_shape=jax.ShapeDtypeStruct((copies, 2 * micro, width), f32),
        compiler_params=params(8),
        name="image_stats",
    )(images)


def combine_stats(arrived, rows, rows_local):
    _, twice, width = arrived.shape

    def kernel(a_ref, out_ref):
        for m in range(twice // 2):
            sums = a_ref[:, 2 * m, :]
            mean = jnp.sum(sums, axis=0, keepdims=True) / rows
            off = sums / rows_local - mean
            squares = jnp.sum(a_ref[:, 2 * m + 1, :], axis=0, keepdims=True)
            squares = squares + rows_local * jnp.sum(off * off, axis=0, keepdims=True)
            out_ref[m, 0:1, :] = mean
            out_ref[m, 1:2, :] = lax.rsqrt(squares / rows + epsilon)

    return pl.pallas_call(
        kernel,
        grid=(1,),
        in_specs=[pl.BlockSpec(arrived.shape, lambda i: (0, 0, 0))],
        out_specs=pl.BlockSpec((twice // 2, 2, width), lambda i: (0, 0, 0)),
        out_shape=jax.ShapeDtypeStruct((twice // 2, 2, width), f32),
        compiler_params=params(8),
        name="combine_stats",
    )(arrived)


small = pl.BlockSpec(memory_space=pltpu.SMEM)
whole = pl.BlockSpec(memory_space=pltpu.VMEM)
kept = pl.BlockSpec(memory_space=pltpu.HBM)
block = 512


def forward(tick, table, images, arrived, stats_img, stats_arr, gain, shift, w_in, w_out, bufs, copies, padded):
    _, rows, width = images.shape
    hidden = w_in.shape[2]
    cuts = [slice(j * block, (j + 1) * block) for j in range(hidden // block)]

    def kernel(at, img, arr, simg, sarr, g, sh, win, wout, *rest):
        rest = rest[len(bufs) :]
        xb, stb, affb, actb, slb, outb, send, part, send_s, part_s, in_s, x_s, st_s, aff_s, act_s, sl_s, w1, w2, sem_x, sem_1, sem_2, sem_o = rest
        came = arr.at[0] if len(arr.shape) == 3 else arr
        slot, first, micro_at = at[3 * tick], at[3 * tick + 1] == 1, at[3 * tick + 2]

        load_1 = [pltpu.make_async_copy(win.at[0, :, c], w1.at[:, c], sem_1.at[j]) for j, c in enumerate(cuts)]
        load_2 = [pltpu.make_async_copy(wout.at[0, c, :], w2.at[c, :], sem_2.at[j]) for j, c in enumerate(cuts)]

        @pl.when(first)
        def _():
            pltpu.make_async_copy(img.at[micro_at], in_s, sem_x).start()

        @pl.when(jnp.logical_not(first))
        def _():
            pltpu.make_async_copy(came, in_s, sem_x).start()

        for load in load_1 + load_2:
            load.start()
        pltpu.make_async_copy(came, in_s, sem_x).wait()
        stores = []

        def store(source, target):
            copy = pltpu.make_async_copy(source, target, sem_o.at[len(stores)])
            copy.start()
            stores.append(copy)

        st = jnp.where(first, simg[pl.ds(micro_at, 1)][0], sarr[0])
        st_s[...] = st
        store(in_s, xb.at[slot])
        store(st_s, stb.at[slot])
        keep_padded(x_s, in_s[...].astype(f32))
        affine = (x_s[...] - st[0:1]) * (st[1:2] * g[...]) + sh[...]
        affine = jnp.where(row_mask(padded, rows), affine, 0.0).astype(bf16)
        aff_s[...] = affine
        store(aff_s, affb.at[slot])

        def first_product(j):
            return jnp.dot(affine, w1[:, cuts[j]], preferred_element_type=f32)

        for load in load_1 + load_2:
            load.wait()
        before = first_product(0)
        for j, c in enumerate(cuts):
            coming = first_product(j + 1) if j + 1 < len(cuts) else None
            value, slope = gelu_parts(before)
            act_s[:, c] = value.astype(bf16)
            sl_s[:, c] = slope.astype(bf16)
            store(act_s.at[:, c], actb.at[slot, :, c])
            store(sl_s.at[:, c], slb.at[slot, :, c])
            before = coming
        grown = jnp.dot(act_s[...], w2[...], preferred_element_type=f32)
        output = (x_s[...] + grown)[:rows].astype(bf16)
        send_s[...] = output
        store(send_s, send)
        fill_copies(part_s, moments(output.astype(f32), rows))
        store(part_s, part)
        store(send_s, outb.at[slot])
        for copy in stores:
            copy.wait()

    out = pl.pallas_call(
        kernel,
        out_shape=[
            pltpu.HBM((3, rows, width), bf16),
            pltpu.HBM((3, 2, width), f32),
            pltpu.HBM((3, padded, width), bf16),
            pltpu.HBM((3, padded, hidden), bf16),
            pltpu.HBM((3, padded, hidden), bf16),
            pltpu.HBM((3, rows, width), bf16),
            pltpu.HBM((rows, width), bf16),
            pltpu.HBM((copies, 2, width), f32),
        ],
        in_specs=[small, kept, kept, whole, whole, whole, whole, kept, kept] + [kept] * len(bufs),
        out_specs=[kept] * 8,
            scratch_shapes=[
                pltpu.VMEM((rows, width), bf16),
                pltpu.VMEM((copies, 2, width), f32),
                pltpu.VMEM((rows, width), bf16),
                pltpu.VMEM((padded, width), f32),
                pltpu.VMEM((2, width), f32),
                pltpu.VMEM((padded, width), bf16),
                pltpu.VMEM((padded, hidden), bf16),
                pltpu.VMEM((padded, hidden), bf16),
                pltpu.VMEM((width, hidden), bf16),
                pltpu.VMEM((hidden, width), bf16),
                pltpu.SemaphoreType.DMA(()),
                pltpu.SemaphoreType.DMA((len(cuts),)),
                pltpu.SemaphoreType.DMA((len(cuts),)),
                pltpu.SemaphoreType.DMA((6 + 2 * len(cuts),)),
            ],
        input_output_aliases={9 + i: i for i in range(len(bufs))},
        compiler_params=params(),
        name="section_forward",
    )(table, images, arrived, stats_img, stats_arr, gain, shift, w_in, w_out, *bufs)
    return list(out[:6]), out[6], out[7]


def backward(tick, table, cotangent, arrived, fix, gain, w_in_t, w_out_t, saved, bufs, copies, padded):
    _, rows, width = cotangent.shape
    hidden = saved[2].shape[2]
    fresh = fix is gain
    cuts = [slice(j * block, (j + 1) * block) for j in range(hidden // block)]

    def kernel(at, cot, arr, fx, g, win, wout, xb, stb, slb, outb, *rest):
        rest = rest[len(bufs) :]
        upb, gbb, ub, send, part, send_s, part_s, in_s, own_s, x_s, st_s, sl_s, pad_s, up_s, keep_s, gb_s, u_s, w1, w2, sem_x, sem_k, sem_1, sem_2, sem_o = rest
        came = arr.at[0] if len(arr.shape) == 3 else arr
        slot, last, micro_at = at[3 * tick], at[3 * tick + 1] == 1, at[3 * tick + 2]

        load_1 = [pltpu.make_async_copy(win.at[0, :, c], w1.at[:, c], sem_1.at[j]) for j, c in enumerate(cuts)]
        load_2 = [pltpu.make_async_copy(wout.at[0, c, :], w2.at[c, :], sem_2.at[j]) for j, c in enumerate(cuts)]

        @pl.when(last)
        def _():
            pltpu.make_async_copy(cot.at[micro_at], in_s, sem_x).start()

        @pl.when(jnp.logical_not(last))
        def _():
            pltpu.make_async_copy(came, in_s, sem_x).start()

        loads = [
            pltpu.make_async_copy(source.at[slot], target, sem_k.at[n])
            for n, (source, target) in enumerate(((outb, own_s), (stb, st_s), (slb, sl_s), (xb, x_s)))
        ]
        for load in [loads[0], load_2[0], loads[2]] + load_2[1:] + loads[1:2] + loads[3:] + load_1:
            load.start()
        pltpu.make_async_copy(came, in_s, sem_x).wait()
        loads[0].wait()
        stores = []

        def store(source, target):
            copy = pltpu.make_async_copy(source, target, sem_o.at[len(stores)])
            copy.start()
            stores.append(copy)

        high = in_s[...].astype(f32)
        if fresh:
            low = jnp.zeros_like(high)
        else:
            low = -fx[0:1] - fx[1:2] * (own_s[...].astype(f32) - fx[2:3])
            low = jnp.where(last, 0.0, low)
        keep_padded(pad_s, high)
        up_s[:padded] = pad_s[...].astype(bf16)
        keep_padded(pad_s, low)
        up_s[padded:] = pad_s[...].astype(bf16)
        u_s[...] = high + low
        keep_s[:, :width] = up_s[:padded]
        keep_s[:, width:] = up_s[padded:]
        store(keep_s, upb.at[slot])

        def first_product(j):
            both = lax.dot_general(up_s[...], w2[cuts[j], :], (((1,), (1,)), ((), ())), preferred_element_type=f32)
            return both[:padded] + both[padded:]

        for load in load_1 + load_2 + loads[1:]:
            load.wait()
        grad_active = first_product(0)
        for j, c in enumerate(cuts):
            coming = first_product(j + 1) if j + 1 < len(cuts) else None
            gb_s[:, c] = (grad_active * sl_s[:, c].astype(f32)).astype(bf16)
            store(gb_s.at[:, c], gbb.at[slot, :, c])
            grad_active = coming
        grad_affine = lax.dot_general(gb_s[...], w1[...], (((1,), (1,)), ((), ())), preferred_element_type=f32)[:rows]
        inverse = st_s[1:2, :]
        normed = (x_s[...].astype(f32) - st_s[0:1, :]) * inverse
        sum_grad = jnp.sum(grad_affine, axis=0, keepdims=True)
        sum_cross = jnp.sum(grad_affine * normed, axis=0, keepdims=True)
        fill_copies(part_s, (sum_grad, sum_cross))
        store(part_s, part)
        u = u_s[...] + inverse * g[...] * grad_affine
        u_s[...] = u
        send_s[...] = u.astype(bf16)
        store(send_s, send)
        store(u_s, ub.at[slot])
        for copy in stores:
            copy.wait()

    out = pl.pallas_call(
        kernel,
        out_shape=[
            pltpu.HBM((3, padded, 2 * width), bf16),
            pltpu.HBM((3, padded, hidden), bf16),
            pltpu.HBM((3, rows, width), f32),
            pltpu.HBM((rows, width), bf16),
            pltpu.HBM((copies, 2, width), f32),
        ],
        in_specs=[small, kept, kept, whole, whole, kept, kept] + [kept] * 4 + [kept] * len(bufs),
        out_specs=[kept] * 5,
            scratch_shapes=[
                pltpu.VMEM((rows, width), bf16),
                pltpu.VMEM((copies, 2, width), f32),
                pltpu.VMEM((rows, width), bf16),
                pltpu.VMEM((rows, width), bf16),
                pltpu.VMEM((rows, width), bf16),
                pltpu.VMEM((2, width), f32),
                pltpu.VMEM((padded, hidden), bf16),
                pltpu.VMEM((padded, width), f32),
                pltpu.VMEM((2 * padded, width), bf16),
                pltpu.VMEM((padded, 2 * width), bf16),
                pltpu.VMEM((padded, hidden), bf16),
                pltpu.VMEM((rows, width), f32),
                pltpu.VMEM((width, hidden), bf16),
                pltpu.VMEM((hidden, width), bf16),
                pltpu.SemaphoreType.DMA(()),
                pltpu.SemaphoreType.DMA((4,)),
                pltpu.SemaphoreType.DMA((len(cuts),)),
                pltpu.SemaphoreType.DMA((len(cuts),)),
                pltpu.SemaphoreType.DMA((4 + len(cuts),)),
            ],
        input_output_aliases={11 + i: i for i in range(len(bufs))},
        compiler_params=params(),
        name="section_backward",
    )(table, cotangent, arrived, fix, gain, w_in_t, w_out_t, *saved, *bufs)
    return list(out[:3]), out[3], out[4]


def combine_grads(tick, table, arrived, stb, gain, rows):
    _, _, width = arrived.shape

    def kernel(at, a_ref, st, g, fix, sums):
        sum_grad = jnp.sum(a_ref[:, 0, :], axis=0, keepdims=True)
        sum_cross = jnp.sum(a_ref[:, 1, :], axis=0, keepdims=True)
        inverse = st[0, 1:2, :]
        scale = inverse * g[...]
        fix[0:1, :] = scale * (sum_grad / rows)
        fix[1:2, :] = scale * inverse * (sum_cross / rows)
        fix[2:3, :] = st[0, 0:1, :]
        sums[0:1, :] = sum_cross
        sums[1:2, :] = sum_grad

    fixed = lambda shape: pl.BlockSpec(shape, lambda j, at: tuple(0 for _ in shape))
    return pl.pallas_call(
        kernel,
        out_shape=[jax.ShapeDtypeStruct((3, width), f32), jax.ShapeDtypeStruct((2, width), f32)],
        grid_spec=pltpu.PrefetchScalarGridSpec(
            num_scalar_prefetch=1,
            grid=(1,),
            in_specs=[
                fixed(arrived.shape),
                pl.BlockSpec((1, 2, width), lambda j, at: (at[3 * tick], 0, 0)),
                fixed((1, width)),
            ],
            out_specs=[fixed((3, width)), fixed((2, width))],
        ),
        compiler_params=params(8),
        name="combine_grads",
    )(table, arrived, stb, gain)


def weight_grad(own_l, other_l, own_r, other_r, terms=1):
    micro, padded, left = own_l.shape
    right = own_r.shape[2] // terms
    block = 512
    steps = right // block

    def kernel(ol, pl_, *rest):
        mine, others, out = rest[:terms], rest[terms:-1], rest[-1]
        contract = (((0,), (0,)), ((), ()))
        dot = lambda a, b: lax.dot_general(a, b, contract, preferred_element_type=f32)
        total = 0.0
        for m in range(micro):
            for k in range(terms):
                total += dot(ol[m], mine[k][m])
                total += dot(pl_[m], others[m * terms + k][...])
        out[...] = total.astype(bf16)

    def mine_at(k):
        return pl.BlockSpec((micro, padded, block), lambda j: (0, 0, j + k * steps))

    def other_at(k):
        return pl.BlockSpec((padded, block), lambda j: (0, j + k * steps))

    return pl.pallas_call(
        kernel,
        grid=(steps,),
        in_specs=[pl.BlockSpec(own_l.shape, lambda j: (0, 0, 0))] * 2
        + [mine_at(k) for k in range(terms)]
        + [other_at(k) for _ in range(micro) for k in range(terms)],
        out_specs=pl.BlockSpec((left, block), lambda j: (0, j)),
        out_shape=jax.ShapeDtypeStruct((left, right), bf16),
        compiler_params=params(),
        name="weight_grad",
    )(own_l, other_l, *[own_r] * terms, *[r for r in other_r for _ in range(terms)])


def half_columns(x, count, core):
    width = x.shape[-1]
    part = width // count
    k = lax.broadcasted_iota(jnp.int32, (width, width // 2), 0)
    n = lax.broadcasted_iota(jnp.int32, (width, width // 2), 1)
    select = (k == (n // part) * (2 * part) + core * part + n % part).astype(bf16)
    return jnp.dot(x, select, preferred_element_type=f32).astype(bf16)


def local(images, cotangent, w_in, w_out, gain, shift):
    sections = lax.axis_size("section")
    replicas = lax.axis_size("dp")
    section = lax.axis_index("section")
    core = lax.axis_index("dp") % 2
    micro, rows_local, _ = images.shape
    rows = rows_local * replicas
    padded = -(-rows_local // 16) * 16
    ticks = micro + sections - 1
    up_route = [(i, i + 1) for i in range(sections - 1)]
    down_route = [(i + 1, i) for i in range(sections - 1)]
    swap_route = [(i, i ^ 1) for i in range(replicas)]

    def exchange(copies):
        return lax.all_to_all(copies, "dp", split_axis=0, concat_axis=0, tiled=True)

    def swap(x):
        return lax.ppermute(x, "dp", swap_route)

    def place(offset, edge, index):
        valid = (offset >= 0) & (offset < micro)
        return [jnp.where(valid, offset, 2), edge.astype(jnp.int32), jnp.int32(index)]

    entries = []
    for tick in range(ticks):
        entries += place(tick - section, section == 0, min(tick, micro - 1))
    for tick in range(ticks):
        entries += place(tick - (sections - 1 - section), section == sections - 1, min(tick, micro - 1))
    table = jnp.stack([e.astype(jnp.int32) for e in entries])
    weights = (w_in, w_out)

    def forward_step(tick, state):
        bufs, sent, part = forward(
            tick, table, images, state["x"], stats_img, state["st"], gain, shift, *weights, state["bufs"], replicas, padded
        )
        state["bufs"] = bufs
        if tick + 1 < ticks:
            everyone = exchange(part)
            state["x"] = lax.ppermute(sent, "section", up_route)
            state["st"] = lax.ppermute(combine_stats(everyone, rows, rows_local), "section", up_route)

    grads = []

    def backward_step(tick, state, back):
        xb, stb, _, _, slb, outb = state["bufs"]
        bufs, sent, part = backward(
            ticks + tick, table, cotangent, back["u"], back["fix"], gain, *weights, (xb, stb, slb, outb), back["bufs"], replicas, padded
        )
        back["bufs"] = bufs
        everyone = exchange(part)
        if tick + 1 < ticks:
            back["u"] = lax.ppermute(sent, "section", down_route)
        fix, sums = combine_grads(ticks + tick, table, everyone, stb, gain, rows)
        grads.append((fix, sums))
        if tick + 1 < ticks:
            back["fix"] = lax.ppermute(fix, "section", down_route)

    stats_img = combine_stats(exchange(image_stats(images, replicas)), rows, rows_local)
    state = {"x": images, "st": stats_img, "bufs": []}
    back = {"u": cotangent, "fix": gain, "bufs": []}
    for tick in range(ticks - 1):
        forward_step(tick, state)
    backward_step(0, state, back)
    forward_step(ticks - 1, state)
    backward_step(1, state, back)
    affb, actb = state["bufs"][2][:micro], state["bufs"][3][:micro]
    own_aff = half_columns(affb, replicas, core)
    other_aff = half_columns(affb, replicas, 1 - core)
    other_act = half_columns(actb, replicas, 1 - core)
    backward_step(2, state, back)
    own_act = half_columns(actb, replicas, core)
    other_aff, other_act = swap(other_aff), swap(other_act)
    for tick in range(3, ticks - 1):
        backward_step(tick, state, back)
    other_up, other_gb = [swap(back["bufs"][0][0])], [swap(back["bufs"][1][0])]
    for tick in range(ticks - 1, ticks):
        backward_step(tick, state, back)
    upb, gbb, ub = back["bufs"]
    for m in range(1, micro):
        other_up.append(swap(upb[m]))
        other_gb.append(swap(gbb[m]))

    groups = [list(range(c, replicas, 2)) for c in range(2)]

    def reduced(part):
        blocks = part.reshape(replicas // 2, -1, part.shape[1])
        got = lax.all_to_all(blocks, "dp", split_axis=0, concat_axis=0, axis_index_groups=groups, tiled=True)
        return got.astype(f32).sum(axis=0)

    reduced_out = reduced(weight_grad(own_act, other_act, upb, other_up, 2))
    reduced_in = reduced(weight_grad(own_aff, other_aff, gbb, other_gb))

    fixes = jnp.stack([g[0] for g in grads])
    sums = jnp.stack([g[1] for g in grads])
    start = sections - 1 - section
    fixes = lax.dynamic_slice_in_dim(fixes, start, micro, 0)
    sums = lax.dynamic_slice_in_dim(sums, start, micro, 0).sum(axis=0)
    x = state["bufs"][0][:micro].astype(f32)
    in_grads = (ub[:micro] - fixes[:, 0:1] - fixes[:, 1:2] * (x - fixes[:, 2:3])).astype(bf16)
    return (
        state["bufs"][5][:micro][None],
        in_grads[None],
        reduced_in[None],
        reduced_out[None],
        sums[0:1],
        sums[1:2],
    )


def solution(mesh):
    placed = (
        P(None, "dp", None),
        P(None, "dp", None),
        P("section", None, None),
        P("section", None, None),
        P("section", None),
        P("section", None),
    )
    return jax.shard_map(
        local,
        mesh=mesh,
        in_specs=placed,
        out_specs=(
            P("section", None, "dp", None),
            P("section", None, "dp", None),
            P("section", "dp", None),
            P("section", "dp", None),
            P("section", None),
            P("section", None),
        ),
        check_vma=False,
    )
```
